32 devices in a mesh: band: 8 (over z, y), grid: 4 (over x, core).
Axes of the slice: x: 2, y: 2, z: 4, core: 2. Of those that a mesh axis runs over, the one named last changes fastest.
Arguments:
- bands: float32 [8, 96, 96, 96], P('band', 'grid'), may hold values from -8 to 8
Outputs:
- exchange_term: float32 [8, 96, 96, 96], P('band', 'grid')
The draws below stay inside these ranges and needn't reach their ends.
All inputs are finite; a program needn't handle non-finite values.
Results may differ from the reference program's by a relative error of at most 0.0003.
Values sent between devices are 32-bit elements; how exact they have to be, the bound alone decides.
No kernel may reach another device: no remote copies, remote signals or barrier semaphores. Data moves between devices by JAX's collectives and lax.ppermute only.
A program may use at most 64 MiB of HBM per device.

```python
import jax
import jax.numpy as jnp
import numpy as np
from jax import lax

NX = 96
NY = 96
NZ = 96
BAND_DEV = 1
CYCLE = 2
BANDS = 8
N_BAND = 8


def draw_bands(key, part):
    full_shape = (BANDS, NX, NY, NZ)
    return jnp.clip(jax.random.normal(key, full_shape, jnp.float32), -6.0, 6.0)


def setup_inputs(seed: int = 0) -> dict:
    keys = jax.random.split(jax.random.key(seed), 2)
    bands = draw_bands(jax.random.fold_in(keys[1], 71), 0)
    return dict(bands=bands)


def wavenumber_sq(indices, length):
    folded = jnp.minimum(indices, length - indices).astype(jnp.float32)
    return (folded * (2.0 * np.pi / length)) * (folded * (2.0 * np.pi / length))


def coulomb(wave_sq, extent):
    screen = 4.0 * np.pi / extent
    guarded = jnp.where(wave_sq > 0, wave_sq, 1.0)
    screened = 0.2 * 4.0 * np.pi / guarded * (1.0 - jnp.exp(-guarded / (4.0 * screen * screen)))
    return jnp.where(wave_sq > 0, screened, 0.0)


def potential(density):
    spectrum = jnp.fft.rfftn(density, axes=(-3, -2, -1))
    wave_sq = (wavenumber_sq(jnp.arange(NX, dtype=jnp.int32), NX)[:, None, None]
               + wavenumber_sq(jnp.arange(NY, dtype=jnp.int32), NY)[None, :, None]
               + wavenumber_sq(jnp.arange(NZ // 2 + 1, dtype=jnp.int32), NZ)[None, None, :])
    return jnp.fft.irfftn(spectrum * coulomb(wave_sq, NX), s=(NX, NY, NZ), axes=(-3, -2, -1))


def reference(bands):
    def one_band(band_id):
        orbital = lax.dynamic_index_in_dim(bands, band_id, 0, keepdims=False)
        owner_block = band_id // BAND_DEV
        summed = jnp.zeros_like(orbital)
        for offset in range(-CYCLE, CYCLE + 1):
            first_row = (((owner_block + offset) % N_BAND) * BAND_DEV).astype(jnp.int32)
            partners = lax.dynamic_slice_in_dim(bands, first_row, BAND_DEV, 0)
            summed = summed + jnp.sum(potential(orbital[None] * partners) * partners, axis=0)
        return -summed

    return lax.map(one_band, jnp.arange(bands.shape[0], dtype=jnp.int32))
```

```python
import functools

import jax
import jax.numpy as jnp
import numpy as np
from jax import lax
from jax.experimental import pallas as pl
from jax.experimental.pallas import tpu as pltpu
from jax.sharding import PartitionSpec as P

CYCLE = 2
LANES = 128
F32 = jnp.float32
BF16 = jnp.bfloat16


def cas(rows, columns, length):
    phases = (np.asarray(rows)[:, None] * np.asarray(columns)[None, :]) % length
    angles = 2.0 * np.pi * phases / length
    return np.cos(angles) + np.sin(angles)


def halves(table):
    high = np.asarray(table, np.float32).astype(jnp.bfloat16)
    low = (np.asarray(table, np.float64) - np.asarray(high, np.float64)).astype(np.float32)
    return high, low.astype(jnp.bfloat16)


class Plan:
    def __init__(self, planes, height, breadth, parts):
        self.planes, self.height, self.breadth, self.parts = planes, height, breadth, parts
        self.length = planes * parts
        self.share = height // parts
        third = breadth // 3
        assert third * 4 == LANES and self.share % 4 == 0 and planes % 8 == 0
        self.third = third
        self.extra = self.share // 4
        self.rows = 3 * self.extra
        assert self.extra <= 8
        self.block = self.rows * planes

    def table_z(self):
        high, low = halves(cas(np.arange(self.breadth), np.arange(self.breadth), self.breadth))
        out = np.zeros((2 * LANES, 2 * LANES), jnp.bfloat16)
        n = self.breadth
        out[:n, :n] = high
        out[:n, LANES : LANES + n] = low
        out[LANES : LANES + n, :n] = high
        return out

    def positions(self, part):
        rows, index = [], []
        for k in range(self.parts):
            base = self.share * (part ^ k)
            for t in range(3):
                for q in range(self.extra):
                    rows.append((k * 3 + t) * 8 + q)
                    index.append(base + t * self.extra + q)
            for q in range(self.extra):
                rows.append((self.parts * 3 + k) * 8 + q)
                index.append(base + 3 * self.extra + q)
        return np.array(rows), np.array(index)

    def table_y(self):
        m = self.parts * 32
        forward, backward = [], []
        for part in range(self.parts):
            rows, index = self.positions(part)
            full = np.zeros((m, self.height))
            full[rows] = cas(index, np.arange(self.height), self.height)
            high, low = halves(full)
            forward.append(np.concatenate([high, high, low], axis=1))
            backward.append(np.concatenate([high.T, high.T, low.T], axis=1))
        return np.stack(forward), np.stack(backward)

    def table_x(self):
        forward, backward = [], []
        for part in range(self.parts):
            order = np.concatenate(
                [np.arange(self.planes) + self.planes * (part ^ k) for k in range(self.parts)]
            )
            high, low = halves(cas(np.arange(self.length), order, self.length))
            forward.append(np.concatenate([high, high, low], axis=1))
            backward.append(np.concatenate([high.T, high.T, low.T], axis=1))
        return np.stack(forward), np.stack(backward)


def split(value):
    high = value.astype(BF16)
    return high, (value - high.astype(F32)).astype(BF16)


def stacked(value):
    high, low = split(value)
    return jnp.concatenate([high, low, high], axis=0)


def dot(a, b):
    return jnp.dot(a, b, preferred_element_type=F32)


def lanes(shape):
    return lax.broadcasted_iota(jnp.int32, shape, len(shape) - 1)


def along_z(value, table):
    high, low = split(value)
    both = dot(jnp.concatenate([high, low], axis=1), table)
    return both[:, :LANES] + both[:, LANES:]


def widen(value):
    rows, width = value.shape
    return jnp.concatenate([value, jnp.zeros((rows, LANES - width), value.dtype)], axis=1)


CHUNK = 8


def forward_kernel(plan, mixed, scalars, *refs):
    if mixed:
        q_ref, r_ref, p_ref, tz_ref, ty_ref, *outs = refs
        even = scalars[1] == 1
    else:
        q_ref, r_ref, tz_ref, ty_ref, *outs = refs
    h, e = plan.height, plan.extra

    def body(step, carry):
        first = step * CHUNK
        a = q_ref[pl.ds(first, CHUNK)]
        b = r_ref[pl.ds(first, CHUNK)]
        if mixed:
            b = jnp.where(even, b, p_ref[pl.ds(first, CHUNK)])
        density = widen((a * b).reshape(CHUNK * h, plan.breadth))
        once = along_z(density, tz_ref[...])
        for pair in range(CHUNK // 2):
            two = jnp.concatenate(
                [once[(2 * pair + i) * h : (2 * pair + i + 1) * h] for i in range(2)], axis=1
            )
            spectrum = dot(ty_ref[0], stacked(two))
            for i in range(2):
                s = spectrum[:, i * LANES : (i + 1) * LANES]
                plane = first + 2 * pair + i
                for k in range(plan.parts):
                    tail = s[(3 * plan.parts + k) * 8 : (3 * plan.parts + k + 1) * 8]
                    for t in range(3):
                        main = s[(k * 3 + t) * 8 : (k * 3 + t + 1) * 8]
                        moved = pltpu.roll(tail, plan.breadth - plan.third * t, 1)
                        packed = jnp.where(lanes(main.shape) < plan.breadth, main, moved)
                        outs[k][pl.ds(t * e * plan.planes + plane, e, stride=plan.planes), :] = (
                            packed[:e]
                        )
        return carry

    lax.fori_loop(0, plan.planes // CHUNK, body, 0)


def middle_kernel(plan, scalars, *refs):
    n = plan.parts
    ins, (filter_ref, tf_ref, tb_ref), outs = refs[:n], refs[n : n + 3], refs[n + 3 :]
    p, length = plan.planes, plan.length

    def body(step, carry):
        row = step * 2
        data = jnp.concatenate(
            [
                jnp.concatenate([ref[pl.ds((row + i) * p, p), :] for ref in ins], axis=0)
                for i in range(2)
            ],
            axis=1,
        )
        spectrum = dot(tf_ref[0], stacked(data))
        screen = jnp.concatenate(
            [filter_ref[pl.ds((row + i) * length, length), :] for i in range(2)], axis=1
        )
        back = dot(tb_ref[0], stacked(spectrum * screen))
        for i in range(2):
            for k in range(n):
                outs[k][pl.ds((row + i) * p, p), :] = back[
                    k * p : (k + 1) * p, i * LANES : (i + 1) * LANES
                ]
        return carry

    lax.fori_loop(0, plan.rows // 2, body, 0)


def pack(value, plan):
    h = plan.height // 4
    wide = widen(value)
    tail = wide[3 * h :]
    parts = []
    for t in range(3):
        main = wide[t * h : (t + 1) * h]
        moved = pltpu.roll(tail, plan.breadth - plan.third * t, 1)
        parts.append(jnp.where(lanes(main.shape) < plan.breadth, main, moved))
    return jnp.concatenate(parts, axis=0)


def unpack(value, plan):
    h = plan.height // 4
    tail = None
    for t in range(3):
        part = value[t * h : (t + 1) * h]
        moved = pltpu.roll(part, (plan.third * (t + 1)) % LANES, 1)
        tail = moved if tail is None else jnp.where(lanes(part.shape) < plan.third * t, tail, moved)
    return jnp.concatenate([value, tail], axis=0)[:, : plan.breadth]


def backward_kernel(plan, kind, scalars, *refs):
    n = plan.parts
    ins, refs = refs[:n], refs[n:]
    tz_ref, ty_ref, *refs = refs
    h, e = plan.height, plan.extra
    even = scalars[1] == 1

    def potential(first):
        planes = []
        for pair in range(CHUNK // 2):
            two = []
            for i in range(2):
                plane = first + 2 * pair + i
                rows, tails = [], []
                for k in range(n):
                    tail = None
                    for t in range(3):
                        part = ins[k][pl.ds(t * e * plan.planes + plane, e, stride=plan.planes), :]
                        part = jnp.concatenate([part, jnp.zeros((8 - e, LANES), F32)], axis=0)
                        rows.append(part)
                        moved = pltpu.roll(part, (plan.third * (t + 1)) % LANES, 1)
                        tail = (
                            moved
                            if tail is None
                            else jnp.where(lanes(part.shape) < plan.third * t, tail, moved)
                        )
                    tails.append(tail)
                two.append(jnp.concatenate(rows + tails, axis=0))
            once = dot(ty_ref[0], stacked(jnp.concatenate(two, axis=1)))
            planes += [once[:, :LANES], once[:, LANES:]]
        value = along_z(jnp.concatenate(planes, axis=0), tz_ref[...])
        return value[:, : plan.breadth].reshape(CHUNK, h, plan.breadth)

    packed_rows = 3 * h // 4

    def store_packed(ref, first, value):
        for i in range(CHUNK):
            ref[pl.ds((first + i) * packed_rows, packed_rows), :] = pack(value[i], plan)

    def body(step, carry):
        first = step * CHUNK
        here = pl.ds(first, CHUNK)
        v = potential(first)
        if kind == "own":
            p_ref, own_ref = refs
            own_ref[here] = v * p_ref[here]
        elif kind == "visit":
            p_ref, r_ref, old_ref, own_ref, away_ref = refs
            own_ref[here] = old_ref[here] + v * r_ref[here]
            away_ref[here] = v * p_ref[here]
        else:
            p_ref, q_ref, r_ref, old_ref, away_ref, own_ref, y_ref, z_ref = refs
            other = v * q_ref[here]
            zero = jnp.zeros_like(other)
            own_ref[here] = old_ref[here] + jnp.where(even, zero, other)
            store_packed(z_ref, first, away_ref[here] + jnp.where(even, other, zero))
            store_packed(y_ref, first, v * jnp.where(even, r_ref[here], p_ref[here]))
        return carry

    lax.fori_loop(0, plan.planes // CHUNK, body, 0)


def final_kernel(plan, scalars, own_ref, y_ref, z_ref, out_ref):
    packed_rows = 3 * plan.height // 4

    def body(plane, carry):
        rows = pl.ds(plane * packed_rows, packed_rows)
        out_ref[plane] = own_ref[plane] + unpack(y_ref[rows, :] + z_ref[rows, :], plan)
        return carry

    lax.fori_loop(0, plan.planes, body, 0)


def call(kernel, scalars, operands, selected, outs, name):
    specs = []
    for i, operand in enumerate(operands):
        if i in selected:
            block = (1,) + operand.shape[1:]
            specs.append(pl.BlockSpec(block, lambda i, s: (s[0], 0, 0)))
        else:
            zeros = (0,) * operand.ndim
            specs.append(pl.BlockSpec(operand.shape, lambda i, s, zeros=zeros: zeros))
    out_specs = [
        pl.BlockSpec(o, lambda i, s, zeros=(0,) * len(o): zeros) for o in outs
    ]
    result = pl.pallas_call(
        kernel,
        grid_spec=pltpu.PrefetchScalarGridSpec(
            num_scalar_prefetch=1, grid=(1,), in_specs=specs, out_specs=out_specs
        ),
        out_shape=[jax.ShapeDtypeStruct(o, F32) for o in outs],
        compiler_params=pltpu.CompilerParams(vmem_limit_bytes=48 * 1024 * 1024),
        name=name,
    )(scalars, *operands)
    return result


def wavenumber_sq(indices, length):
    folded = jnp.minimum(indices, length - indices).astype(F32)
    return folded * (2.0 * np.pi / length) * (folded * (2.0 * np.pi / length))


def coulomb(wave_sq, extent):
    screen = 4.0 * np.pi / extent
    guarded = jnp.where(wave_sq > 0, wave_sq, 1.0)
    screened = 0.2 * 4.0 * np.pi / guarded * (1.0 - jnp.exp(-guarded / (4.0 * screen * screen)))
    return jnp.where(wave_sq > 0, screened, 0.0)


def screen_of(plan, part):
    shape = (plan.rows, plan.length, LANES)
    row = lax.broadcasted_iota(jnp.int32, shape, 0)
    lane = lax.broadcasted_iota(jnp.int32, shape, 2)
    main = lane < plan.breadth
    index_y = part * plan.share + jnp.where(main, row, 3 * plan.extra + row % plan.extra)
    index_z = jnp.where(main, lane, plan.third * (row // plan.extra) + lane - plan.breadth)
    wave_sq = (
        wavenumber_sq(lax.broadcasted_iota(jnp.int32, shape, 1), plan.length)
        + wavenumber_sq(index_y, plan.height)
        + wavenumber_sq(index_z, plan.breadth)
    )
    cells = plan.length * plan.height * plan.breadth
    return (coulomb(wave_sq, plan.length) * (-1.0 / cells)).reshape(-1, LANES)


def exchange(blocks, parts):
    return [blocks[0]] + [
        lax.ppermute(blocks[k], "grid", [(i, i ^ k) for i in range(parts)])
        for k in range(1, parts)
    ]


def shards(bands):
    parts = lax.axis_size("grid")
    number = lax.axis_size("band")
    own = bands[0]
    plan = Plan(*own.shape, parts)
    part = lax.axis_index("grid")
    even = 1 - lax.axis_index("band") % 2
    scalars = jnp.stack([part, even]).astype(jnp.int32)
    swap = [(i, i ^ 1) for i in range(number)]
    q = lax.ppermute(own, "band", swap)
    r = lax.ppermute(own, "band", [(i, (i - CYCLE) % number) for i in range(number)])
    tz = jnp.asarray(plan.table_z())
    ty_forward, ty_backward = (jnp.asarray(t) for t in plan.table_y())
    tx_forward, tx_backward = (jnp.asarray(t) for t in plan.table_x())
    screen = screen_of(plan, part)
    block = (plan.block, LANES)
    whole = own.shape
    packed = (plan.planes * 3 * plan.height // 4, LANES)

    def forward(*fields):
        n = len(fields)
        return call(
            functools.partial(forward_kernel, plan, n == 3),
            scalars,
            (*fields, tz, ty_forward),
            (n + 1,),
            [block] * parts,
            "forward",
        )

    def middle(blocks):
        return call(
            functools.partial(middle_kernel, plan),
            scalars,
            (*blocks, screen, tx_forward, tx_backward),
            (parts + 1, parts + 2),
            [block] * parts,
            "middle",
        )

    def backward(kind, blocks, fields, outs):
        return call(
            functools.partial(backward_kernel, plan, kind),
            scalars,
            (*blocks, tz, ty_backward, *fields),
            (parts + 1,),
            outs,
            kind,
        )

    def solved(*fields):
        return exchange(middle(exchange(forward(*fields), parts)), parts)

    pair_own = solved(own, own)
    pair_visit = solved(own, r)
    pair_mixed = solved(q, r, own)
    (total,) = backward("own", pair_own, (own,), [whole])
    total, away = backward("visit", pair_visit, (own, r, total), [whole, whole])
    total, to_y, to_z = backward(
        "mixed", pair_mixed, (own, q, r, total, away), [whole, packed, packed]
    )
    from_y = lax.ppermute(to_y, "band", swap)
    from_z = lax.ppermute(to_z, "band", [(i, (i + CYCLE) % number) for i in range(number)])
    (result,) = call(
        functools.partial(final_kernel, plan), scalars, (total, from_y, from_z), (), [whole], "final"
    )
    return result[None]


def solution(mesh):
    return jax.shard_map(
        shards,
        mesh=mesh,
        in_specs=(P("band", "grid", None, None),),
        out_specs=P("band", "grid", None, None),
        check_vma=False,
    )
```

```python
import functools

import jax
import jax.numpy as jnp
import numpy as np
from jax import lax
from jax.experimental import pallas as pl
from jax.experimental.pallas import tpu as pltpu
from jax.sharding import PartitionSpec as P


CYCLE = 2
LANES = 128
F32 = jnp.float32
BF16 = jnp.bfloat16


def cas(rows, columns, length):
    phases = (np.asarray(rows)[:, None] * np.asarray(columns)[None, :]) % length
    angles = 2.0 * np.pi * phases / length
    return np.cos(angles) + np.sin(angles)


def halves(table):
    high = np.asarray(table, np.float32).astype(jnp.bfloat16)
    low = (np.asarray(table, np.float64) - np.asarray(high, np.float64)).astype(np.float32)
    return high, low.astype(jnp.bfloat16)


def doubled(high, low):
    return np.concatenate(
        [np.concatenate([high, high], axis=1), np.concatenate([low, np.zeros_like(low)], axis=1)],
        axis=0,
    )


def wavenumber_sq(indices, length):
    folded = np.minimum(indices, length - indices).astype(np.float32)
    scaled = folded * np.float32(2.0 * np.pi / length)
    return scaled * scaled


class Plan:
    def __init__(self, planes, height, breadth, parts):
        self.planes, self.height, self.breadth, self.parts = planes, height, breadth, parts
        self.length = planes * parts
        self.share = height // parts
        third = breadth // 3
        assert third * 4 == LANES and self.share % 4 == 0 and planes % 8 == 0
        self.third = third
        self.extra = self.share // 4
        self.rows = 3 * self.extra
        assert self.extra <= 8
        self.block = self.rows * planes

    def table_z(self):
        high, low = halves(cas(np.arange(self.breadth), np.arange(self.breadth), self.breadth))
        out = np.zeros((2 * LANES, 2 * LANES), jnp.bfloat16)
        n = self.breadth
        out[:n, :n] = high
        out[:n, LANES : LANES + n] = low
        out[LANES : LANES + n, :n] = high
        return out

    def positions(self, part):
        rows, index = [], []
        for k in range(self.parts):
            base = self.share * (part ^ k)
            for t in range(3):
                for q in range(self.extra):
                    rows.append((k * 3 + t) * 8 + q)
                    index.append(base + t * self.extra + q)
            for q in range(self.extra):
                rows.append((self.parts * 3 + k) * 8 + q)
                index.append(base + 3 * self.extra + q)
        return np.array(rows), np.array(index)

    def table_y(self):
        m = self.parts * 32
        forward, backward = [], []
        for part in range(self.parts):
            rows, index = self.positions(part)
            full = np.zeros((m, self.height))
            full[rows] = cas(index, np.arange(self.height), self.height)
            high, low = halves(full)
            forward.append(doubled(high, low))
            backward.append(doubled(high.T, low.T))
        return np.stack(forward), np.stack(backward)

    def table_x(self):
        forward, backward = [], []
        for part in range(self.parts):
            order = np.concatenate(
                [np.arange(self.planes) + self.planes * (part ^ k) for k in range(self.parts)]
            )
            high, low = halves(cas(np.arange(self.length), order, self.length))
            forward.append(doubled(high, low))
            backward.append(doubled(high.T, low.T))
        return np.stack(forward), np.stack(backward)

    def waves(self):
        across = np.broadcast_to(
            wavenumber_sq(np.arange(self.length), self.length)[:, None], (self.length, LANES)
        )
        row = np.arange(self.rows)[:, None]
        lane = np.arange(LANES)[None, :]
        main = lane < self.breadth
        y = np.where(main, row, 3 * self.extra + row % self.extra)
        z = np.where(main, lane, self.third * (row // self.extra) + lane - self.breadth)
        within = np.zeros((self.parts, -(-self.rows // 8) * 8, LANES), np.float32)
        for part in range(self.parts):
            within[part, : self.rows] = wavenumber_sq(
                part * self.share + y, self.height
            ) + wavenumber_sq(z, self.breadth)
        return np.array(across), within


def split(value):
    high = value.astype(BF16)
    return high, (value - high.astype(F32)).astype(BF16)


def dot(a, b):
    return jnp.dot(a, b, preferred_element_type=F32)


def lanes(shape):
    return lax.broadcasted_iota(jnp.int32, shape, len(shape) - 1)


def along_rows(table, value):
    both = dot(table, jnp.concatenate(split(value), axis=0))
    half = both.shape[0] // 2
    return both[:half] + both[half:]


def along_lanes(value, table):
    both = dot(jnp.concatenate(split(value), axis=1), table)
    return both[:, :LANES] + both[:, LANES:]


def widen(value):
    rows, width = value.shape
    return jnp.concatenate([value, jnp.zeros((rows, LANES - width), value.dtype)], axis=1)


def pack(wide, plan):
    h = plan.height // 4
    tail = wide[3 * h :]
    parts = []
    for t in range(3):
        main = wide[t * h : (t + 1) * h]
        moved = pltpu.roll(tail, plan.breadth - plan.third * t, 1)
        parts.append(jnp.where(lanes(main.shape) < plan.breadth, main, moved))
    return jnp.concatenate(parts, axis=0)


def thirds(parts, plan):
    tail = None
    for t, part in enumerate(parts):
        moved = pltpu.roll(part, (plan.third * (t + 1)) % LANES, 1)
        tail = moved if tail is None else jnp.where(lanes(part.shape) < plan.third * t, tail, moved)
    return tail


def unpack(value, plan):
    h = plan.height // 4
    return jnp.concatenate(
        [value, thirds([value[t * h : (t + 1) * h] for t in range(3)], plan)], axis=0
    )


def clear(wide, plan):
    return jnp.where(lanes(wide.shape) < plan.breadth, wide, 0.0)


def store_spectrum(plan, density, tz, ty, outs, base, stride, plane):
    h, e = plan.height, plan.extra
    once = along_lanes(density, tz)
    for pair in range(CHUNK // 2):
        two = jnp.concatenate(
            [once[(2 * pair + i) * h : (2 * pair + i + 1) * h] for i in range(2)], axis=1
        )
        spectrum = along_rows(ty, two)
        for i in range(2):
            s = spectrum[:, i * LANES : (i + 1) * LANES]
            for k in range(plan.parts):
                tail = s[(3 * plan.parts + k) * 8 : (3 * plan.parts + k + 1) * 8]
                for t in range(3):
                    main = s[(k * 3 + t) * 8 : (k * 3 + t + 1) * 8]
                    moved = pltpu.roll(tail, plan.breadth - plan.third * t, 1)
                    packed = jnp.where(lanes(main.shape) < plan.breadth, main, moved)
                    first = base + t * e * stride + plane + 2 * pair + i
                    outs[k][pl.ds(first, e, stride=stride), :] = packed[:e]


def load_potential(plan, ins, base, stride, plane, tz, ty):
    e = plan.extra
    planes = []
    for pair in range(CHUNK // 2):
        two = []
        for i in range(2):
            rows, tails = [], []
            for k in range(plan.parts):
                parts = []
                for t in range(3):
                    first = base + t * e * stride + plane + 2 * pair + i
                    part = ins[k][pl.ds(first, e, stride=stride), :]
                    parts.append(jnp.concatenate([part, jnp.zeros((8 - e, LANES), F32)], axis=0))
                rows += parts
                tails.append(thirds(parts, plan))
            two.append(jnp.concatenate(rows + tails, axis=0))
        once = along_rows(ty, jnp.concatenate(two, axis=1))
        planes += [once[:, :LANES], once[:, LANES:]]
    return along_lanes(jnp.concatenate(planes, axis=0), tz)


CHUNK = 8


def forward_own_kernel(plan, scalars, own_ref, tz_ref, ty_ref, *outs):
    blocks, chunks = outs[: plan.parts], outs[plan.parts :]
    h = plan.height
    packed_rows = 3 * h // 4
    for c, chunk in enumerate(chunks):
        own = own_ref[c * CHUNK : (c + 1) * CHUNK].reshape(CHUNK * h, plan.breadth)
        wide = widen(own)
        for i in range(CHUNK):
            chunk[i * packed_rows : (i + 1) * packed_rows, :] = pack(
                wide[i * h : (i + 1) * h], plan
            )
        store_spectrum(plan, wide * wide, tz_ref[...], ty_ref[0], blocks, 0, plan.planes, c * CHUNK)


def load_packed(ref, plan):
    packed_rows = 3 * plan.height // 4
    return jnp.concatenate(
        [unpack(ref[i * packed_rows : (i + 1) * packed_rows, :], plan) for i in range(CHUNK)],
        axis=0,
    )


def load_own(ref, plan):
    return widen(ref[...].reshape(CHUNK * plan.height, plan.breadth))


def forward_pair_kernel(plan, scalars, own_ref, q_ref, r_ref, tz_ref, ty_ref, after_ref, *outs):
    even = scalars[1] == 1
    p = load_own(own_ref, plan)
    r = load_packed(r_ref, plan)
    tz, ty = tz_ref[...], ty_ref[0]
    store_spectrum(plan, p * r, tz, ty, outs, 0, CHUNK, 0)
    q = load_packed(q_ref, plan)
    mixed = clear(q * jnp.where(even, r, p), plan)
    store_spectrum(plan, mixed, tz, ty, outs, plan.rows * CHUNK, CHUNK, 0)


def screen_kernel(plan, scalars, across_ref, within_ref, after_ref, out_ref):
    cells = plan.length * plan.height * plan.breadth
    limit = 4.0 * np.pi / plan.length
    rate = 1.0 / (4.0 * limit * limit)
    for row in range(plan.rows):
        wave_sq = across_ref[...] + within_ref[0, row : row + 1, :]
        guarded = jnp.where(wave_sq > 0, wave_sq, 1.0)
        screened = (-0.2 * 4.0 * np.pi / cells) / guarded * (1.0 - jnp.exp(guarded * -rate))
        out_ref[row * plan.length : (row + 1) * plan.length, :] = jnp.where(
            wave_sq > 0, screened, 0.0
        )


def middle_kernel(plan, sizes_in, sizes_out, count, scalars, *refs):
    n = plan.parts
    ins = [refs[k * len(sizes_in) : (k + 1) * len(sizes_in)] for k in range(n)]
    refs = refs[n * len(sizes_in) :]
    screen_ref, tf_ref, tb_ref, after_ref, *refs = refs
    outs = [refs[k * len(sizes_out) : (k + 1) * len(sizes_out)] for k in range(n)]
    length = plan.length
    for pair in range(plan.rows // 2):
        for solve in range(count):
            columns = []
            for i in range(2):
                row = pair * 2 + i
                parts = []
                for k in range(n):
                    for ref, size in zip(ins[k], sizes_in):
                        first = (solve * plan.rows + row) * size
                        parts.append(ref[first : first + size, :])
                columns.append(jnp.concatenate(parts, axis=0))
            spectrum = along_rows(tf_ref[0], jnp.concatenate(columns, axis=1))
            screen = jnp.concatenate(
                [
                    screen_ref[(pair * 2 + i) * length : (pair * 2 + i + 1) * length, :]
                    for i in range(2)
                ],
                axis=1,
            )
            back = along_rows(tb_ref[0], spectrum * screen)
            for i in range(2):
                row = pair * 2 + i
                for k in range(n):
                    at = k * plan.planes
                    for ref, size in zip(outs[k], sizes_out):
                        first = (solve * plan.rows + row) * size
                        ref[first : first + size, :] = back[
                            at : at + size, i * LANES : (i + 1) * LANES
                        ]
                        at += size


def backward_pair_kernel(plan, scalars, *refs):
    n = plan.parts
    ins, refs = refs[:n], refs[n:]
    own_ref, q_ref, r_ref, tz_ref, ty_ref, _, total_ref, y_ref, z_ref = refs
    even = scalars[1] == 1
    h = plan.height
    tz, ty = tz_ref[...], ty_ref[0]
    visit = load_potential(plan, ins, 0, CHUNK, 0, tz, ty)
    mixed = load_potential(plan, ins, plan.rows * CHUNK, CHUNK, 0, tz, ty)
    p = load_own(own_ref, plan)
    r = load_packed(r_ref, plan)
    q = load_packed(q_ref, plan)
    other = mixed * q
    zero = jnp.zeros_like(other)
    total = visit * r + jnp.where(even, zero, other)
    total_ref[...] = total[:, : plan.breadth].reshape(CHUNK, h, plan.breadth)
    to_z = visit * p + jnp.where(even, other, zero)
    to_y = mixed * jnp.where(even, r, p)
    packed_rows = 3 * h // 4
    for i in range(CHUNK):
        rows = slice(i * packed_rows, (i + 1) * packed_rows)
        y_ref[rows, :] = pack(to_y[i * h : (i + 1) * h], plan)
        z_ref[rows, :] = pack(to_z[i * h : (i + 1) * h], plan)


def backward_own_kernel(plan, sizes, scalars, *refs):
    n, m = plan.parts, len(sizes)
    ins = [refs[k * m : (k + 1) * m] for k in range(n)]
    refs = refs[n * m :]
    chunks = plan.planes // CHUNK
    totals, refs = refs[:chunks], refs[chunks:]
    own_ref, tz_ref, ty_ref, _, out_ref = refs
    for c in range(chunks):
        at, piece = c * CHUNK, 0
        while at >= sizes[piece]:
            at -= sizes[piece]
            piece += 1
        value = load_potential(
            plan, [ins[k][piece] for k in range(n)], 0, sizes[piece], at, tz_ref[...], ty_ref[0]
        )
        value = value[:, : plan.breadth].reshape(CHUNK, plan.height, plan.breadth)
        here = slice(c * CHUNK, (c + 1) * CHUNK)
        out_ref[here] = totals[c][...] + value * own_ref[here]


def final_kernel(plan, scalars, own_ref, *refs):
    chunks = plan.planes // CHUNK
    ys, zs, out_ref = refs[:chunks], refs[chunks : 2 * chunks], refs[-1]
    packed_rows = 3 * plan.height // 4
    for c in range(chunks):
        for i in range(CHUNK):
            rows = slice(i * packed_rows, (i + 1) * packed_rows)
            returned = unpack(ys[c][rows, :] + zs[c][rows, :], plan)
            out_ref[c * CHUNK + i] = own_ref[c * CHUNK + i] + returned[:, : plan.breadth]


def call(kernel, scalars, operands, outs, selected=(), chunk=None, after=None):
    specs = []
    for operand in operands:
        if any(operand is s for s in selected):
            specs.append(pl.BlockSpec((1,) + operand.shape[1:], lambda i, s: (s[0], 0, 0)))
        elif chunk is not None and operand is chunk[0]:
            specs.append(
                pl.BlockSpec(
                    (CHUNK,) + operand.shape[1:], lambda i, s, c=chunk[1]: (c, 0, 0)
                )
            )
        else:
            zeros = (0,) * operand.ndim
            specs.append(pl.BlockSpec(operand.shape, lambda i, s, zeros=zeros: zeros))
    if after is not None:
        operands = (*operands, after)
        specs.append(pl.BlockSpec(memory_space=pl.ANY))
    out_specs = [pl.BlockSpec(o, lambda i, s, zeros=(0,) * len(o): zeros) for o in outs]
    return pl.pallas_call(
        kernel,
        grid_spec=pltpu.PrefetchScalarGridSpec(
            num_scalar_prefetch=1, grid=(1,), in_specs=specs, out_specs=out_specs
        ),
        out_shape=[jax.ShapeDtypeStruct(o, F32) for o in outs],
        compiler_params=pltpu.CompilerParams(vmem_limit_bytes=48 * 1024 * 1024),
    )(scalars, *operands)


def exchange(blocks, parts):
    return [blocks[0]] + [
        lax.ppermute(blocks[k], "grid", [(i, i ^ k) for i in range(parts)])
        for k in range(1, parts)
    ]


def exchange_term(bands):
    parts = lax.axis_size("grid")
    number = lax.axis_size("band")
    own = bands[0]
    plan = Plan(*own.shape, parts)
    part = lax.axis_index("grid")
    even = 1 - lax.axis_index("band") % 2
    scalars = jnp.stack([part, even]).astype(jnp.int32)
    swap = [(i, i ^ 1) for i in range(number)]
    behind = [(i, (i - CYCLE) % number) for i in range(number)]
    ahead = [(i, (i + CYCLE) % number) for i in range(number)]
    tz = jnp.asarray(plan.table_z())
    ty_forward, ty_backward = (jnp.asarray(t) for t in plan.table_y())
    tx_forward, tx_backward = (jnp.asarray(t) for t in plan.table_x())
    across, within = (jnp.asarray(t) for t in plan.waves())
    chunks = plan.planes // CHUNK
    whole = own.shape
    packed = (CHUNK * 3 * plan.height // 4, LANES)
    sizes = (CHUNK, plan.planes - CHUNK)

    *blocks, = call(
        functools.partial(forward_own_kernel, plan),
        scalars,
        (own, tz, ty_forward),
        [(plan.block, LANES)] * parts + [packed] * chunks,
        (ty_forward,),
    )
    blocks, mine = blocks[:parts], blocks[parts:]
    own_in = exchange(blocks, parts)
    q, r = [], []
    for chunk in mine:
        r.append(lax.ppermute(chunk, "band", behind))
        q.append(lax.ppermute(chunk, "band", swap))
    (screen,) = call(
        functools.partial(screen_kernel, plan),
        scalars,
        (across, within),
        [(plan.rows * plan.length, LANES)],
        (within,),
        after=blocks[0],
    )
    after = screen
    pair_in = []
    for c in range(chunks):
        out = call(
            functools.partial(forward_pair_kernel, plan),
            scalars,
            (own, q[c], r[c], tz, ty_forward),
            [(2 * plan.rows * CHUNK, LANES)] * parts,
            (ty_forward,),
            (own, c),
            after,
        )
        after = out[0]
        pair_in.append(exchange(out, parts))

    def middle(ins, sizes_in, sizes_out, count, after):
        out = call(
            functools.partial(middle_kernel, plan, sizes_in, sizes_out, count),
            scalars,
            (*[block for part in ins for block in part], screen, tx_forward, tx_backward),
            [(count * plan.rows * size, LANES) for size in sizes_out] * parts,
            (tx_forward, tx_backward),
            after=after,
        )
        return [out[i :: len(sizes_out)] for i in range(len(sizes_out))]

    own_mid = middle([[b] for b in own_in], (plan.planes,), sizes, 1, after)
    own_back = [exchange(own_mid[0], parts)]
    even_chunks = (CHUNK,) * chunks
    pair_mid = middle(
        [[pair_in[c][k] for c in range(chunks)] for k in range(parts)],
        even_chunks,
        even_chunks,
        2,
        own_mid[0][0],
    )
    pair_back = [exchange(blocks, parts) for blocks in pair_mid]
    own_back.append(exchange(own_mid[1], parts))
    after = pair_mid[0][0]
    totals, from_y, from_z = [], [], []
    for c in range(chunks):
        total, y, z = call(
            functools.partial(backward_pair_kernel, plan),
            scalars,
            (*pair_back[c], own, q[c], r[c], tz, ty_backward),
            [(CHUNK,) + whole[1:], packed, packed],
            (ty_backward,),
            (own, c),
            after,
        )
        after = total
        totals.append(total)
        from_z.append(lax.ppermute(z, "band", ahead))
        from_y.append(lax.ppermute(y, "band", swap))
    (total,) = call(
        functools.partial(backward_own_kernel, plan, sizes),
        scalars,
        (*[own_back[i][k] for k in range(parts) for i in range(2)], *totals, own, tz, ty_backward),
        [whole],
        (ty_backward,),
        after=after,
    )
    (result,) = call(
        functools.partial(final_kernel, plan), scalars, (total, *from_y, *from_z), [whole]
    )
    return result[None]


def solution(mesh):
    return jax.shard_map(
        exchange_term,
        mesh=mesh,
        in_specs=(P("band", "grid", None, None),),
        out_specs=P("band", "grid", None, None),
        check_vma=False,
    )
```

```python
import functools

import jax
import jax.numpy as jnp
import numpy as np
from jax import lax
from jax.experimental import pallas as pl
from jax.experimental.pallas import tpu as pltpu
from jax.sharding import PartitionSpec as P


CYCLE = 2
LANES = 128
F32 = jnp.float32
BF16 = jnp.bfloat16


def cas(rows, columns, length):
    phases = (np.asarray(rows)[:, None] * np.asarray(columns)[None, :]) % length
    angles = 2.0 * np.pi * phases / length
    return np.cos(angles) + np.sin(angles)


def halves(table):
    high = np.asarray(table, np.float32).astype(jnp.bfloat16)
    low = (np.asarray(table, np.float64) - np.asarray(high, np.float64)).astype(np.float32)
    return high, low.astype(jnp.bfloat16)


def doubled(high, low):
    return np.concatenate(
        [np.concatenate([high, high], axis=1), np.concatenate([low, np.zeros_like(low)], axis=1)],
        axis=0,
    )


def wavenumber_sq(indices, length):
    folded = np.minimum(indices, length - indices).astype(np.float32)
    scaled = folded * np.float32(2.0 * np.pi / length)
    return scaled * scaled


class Plan:
    def __init__(self, planes, height, breadth, parts):
        self.planes, self.height, self.breadth, self.parts = planes, height, breadth, parts
        self.length = planes * parts
        self.share = height // parts
        third = breadth // 3
        assert third * 4 == LANES and self.share % 4 == 0 and planes % 8 == 0
        self.third = third
        self.extra = self.share // 4
        self.rows = 3 * self.extra
        assert self.extra <= 8
        self.block = self.rows * planes
        self.packed = 3 * height // 4

    def table_z(self):
        high, low = halves(cas(np.arange(self.breadth), np.arange(self.breadth), self.breadth))
        out = np.zeros((2 * LANES, 2 * LANES), jnp.bfloat16)
        n = self.breadth
        out[:n, :n] = high
        out[:n, LANES : LANES + n] = low
        out[LANES : LANES + n, :n] = high
        return out

    def positions(self, part):
        rows, index = [], []
        for k in range(self.parts):
            base = self.share * (part ^ k)
            for t in range(3):
                for q in range(self.extra):
                    rows.append((k * 3 + t) * 8 + q)
                    index.append(base + t * self.extra + q)
            for q in range(self.extra):
                rows.append((self.parts * 3 + k) * 8 + q)
                index.append(base + 3 * self.extra + q)
        return np.array(rows), np.array(index)

    def table_y(self):
        m = self.parts * 32
        forward, backward = [], []
        for part in range(self.parts):
            rows, index = self.positions(part)
            full = np.zeros((m, self.height))
            full[rows] = cas(index, np.arange(self.height), self.height)
            high, low = halves(full)
            forward.append(doubled(high, low))
            backward.append(doubled(high.T, low.T))
        return np.stack(forward), np.stack(backward)

    def table_x(self):
        forward, backward = [], []
        for part in range(self.parts):
            order = np.concatenate(
                [np.arange(self.planes) + self.planes * (part ^ k) for k in range(self.parts)]
            )
            high, low = halves(cas(np.arange(self.length), order, self.length))
            forward.append(doubled(high, low))
            backward.append(doubled(high.T, low.T))
        return np.stack(forward), np.stack(backward)

    def waves(self):
        across = np.broadcast_to(
            wavenumber_sq(np.arange(self.length), self.length)[:, None], (self.length, LANES)
        )
        row = np.arange(self.rows)[:, None]
        lane = np.arange(LANES)[None, :]
        main = lane < self.breadth
        y = np.where(main, row, 3 * self.extra + row % self.extra)
        z = np.where(main, lane, self.third * (row // self.extra) + lane - self.breadth)
        within = np.zeros((self.parts, -(-self.rows // 8) * 8, LANES), np.float32)
        for part in range(self.parts):
            within[part, : self.rows] = wavenumber_sq(
                part * self.share + y, self.height
            ) + wavenumber_sq(z, self.breadth)
        return np.array(across), within


def split(value):
    high = value.astype(BF16)
    return high, (value - high.astype(F32)).astype(BF16)


def dot(a, b):
    return jnp.dot(a, b, preferred_element_type=F32)


def lanes(shape):
    return lax.broadcasted_iota(jnp.int32, shape, len(shape) - 1)


def along_rows(table, value):
    both = dot(table, jnp.concatenate(split(value), axis=0))
    half = both.shape[0] // 2
    return both[:half] + both[half:]


def along_lanes(value, table):
    both = dot(jnp.concatenate(split(value), axis=1), table)
    return both[:, :LANES] + both[:, LANES:]


def widen(value):
    rows, width = value.shape
    return jnp.concatenate([value, jnp.zeros((rows, LANES - width), value.dtype)], axis=1)


def pack(wide, plan):
    h = plan.height // 4
    tail = wide[3 * h :]
    parts = []
    for t in range(3):
        main = wide[t * h : (t + 1) * h]
        moved = pltpu.roll(tail, plan.breadth - plan.third * t, 1)
        parts.append(jnp.where(lanes(main.shape) < plan.breadth, main, moved))
    return jnp.concatenate(parts, axis=0)


def thirds(parts, plan):
    tail = None
    for t, part in enumerate(parts):
        moved = pltpu.roll(part, (plan.third * (t + 1)) % LANES, 1)
        tail = moved if tail is None else jnp.where(lanes(part.shape) < plan.third * t, tail, moved)
    return tail


def unpack(value, plan):
    h = plan.height // 4
    return jnp.concatenate(
        [value, thirds([value[t * h : (t + 1) * h] for t in range(3)], plan)], axis=0
    )


def store_spectrum(plan, density, tz, ty, outs, base, stride, plane):
    h, e = plan.height, plan.extra
    once = along_lanes(density, tz)
    for pair in range(CHUNK // 2):
        two = jnp.concatenate(
            [once[(2 * pair + i) * h : (2 * pair + i + 1) * h] for i in range(2)], axis=1
        )
        spectrum = along_rows(ty, two)
        for i in range(2):
            s = spectrum[:, i * LANES : (i + 1) * LANES]
            for k in range(plan.parts):
                tail = s[(3 * plan.parts + k) * 8 : (3 * plan.parts + k + 1) * 8]
                for t in range(3):
                    main = s[(k * 3 + t) * 8 : (k * 3 + t + 1) * 8]
                    moved = pltpu.roll(tail, plan.breadth - plan.third * t, 1)
                    packed = jnp.where(lanes(main.shape) < plan.breadth, main, moved)
                    first = base + t * e * stride + plane + 2 * pair + i
                    outs[k][pl.ds(first, e, stride=stride), :] = packed[:e]


def load_potential(plan, ins, base, stride, plane, tz, ty):
    e = plan.extra
    planes = []
    for pair in range(CHUNK // 2):
        two = []
        for i in range(2):
            rows, tails = [], []
            for k in range(plan.parts):
                parts = []
                for t in range(3):
                    first = base + t * e * stride + plane + 2 * pair + i
                    part = ins[k][pl.ds(first, e, stride=stride), :]
                    parts.append(jnp.concatenate([part, jnp.zeros((8 - e, LANES), F32)], axis=0))
                rows += parts
                tails.append(thirds(parts, plan))
            two.append(jnp.concatenate(rows + tails, axis=0))
        once = along_rows(ty, jnp.concatenate(two, axis=1))
        planes += [once[:, :LANES], once[:, LANES:]]
    return along_lanes(jnp.concatenate(planes, axis=0), tz)


CHUNK = 8


def pack_kernel(plan, scalars, own_ref, out):
    for i in range(CHUNK):
        out[i * plan.packed : (i + 1) * plan.packed, :] = pack(widen(own_ref[i]), plan)


def unpack_chunk(value, plan):
    return jnp.concatenate(
        [unpack(value[i * plan.packed : (i + 1) * plan.packed], plan) for i in range(CHUNK)],
        axis=0,
    )


def pack_chunk(wide, plan):
    h = plan.height
    return jnp.concatenate(
        [pack(wide[i * h : (i + 1) * h], plan) for i in range(CHUNK)], axis=0
    )


def forward_own_kernel(plan, scalars, own_ref, tz_ref, ty_ref, after_ref, *outs):
    blocks, later = outs[: plan.parts], outs[plan.parts :]
    for c in range(plan.planes // CHUNK):
        here = slice(c * CHUNK, (c + 1) * CHUNK)
        wide = widen(own_ref[here].reshape(CHUNK * plan.height, plan.breadth))
        if c:
            later[c - 1][...] = pack_chunk(wide, plan)
        store_spectrum(
            plan, wide * wide, tz_ref[...], ty_ref[0], blocks, 0, plan.planes, c * CHUNK
        )


def forward_pair_kernel(plan, scalars, p_ref, q_ref, r_ref, tz_ref, ty_ref, after_ref, *outs):
    even = scalars[1] == 1
    p, r = p_ref[...], r_ref[...]
    tz, ty = tz_ref[...], ty_ref[0]
    store_spectrum(plan, unpack_chunk(p * r, plan), tz, ty, outs, 0, CHUNK, 0)
    mixed = q_ref[...] * jnp.where(even, r, p)
    store_spectrum(plan, unpack_chunk(mixed, plan), tz, ty, outs, plan.rows * CHUNK, CHUNK, 0)


def screen_kernel(plan, scalars, across_ref, within_ref, after_ref, out_ref):
    cells = plan.length * plan.height * plan.breadth
    limit = 4.0 * np.pi / plan.length
    rate = 1.0 / (4.0 * limit * limit)
    for row in range(plan.rows):
        wave_sq = across_ref[...] + within_ref[0, row : row + 1, :]
        guarded = jnp.where(wave_sq > 0, wave_sq, 1.0)
        screened = (-0.2 * 4.0 * np.pi / cells) / guarded * (1.0 - jnp.exp(guarded * -rate))
        out_ref[row * plan.length : (row + 1) * plan.length, :] = jnp.where(
            wave_sq > 0, screened, 0.0
        )


def middle_kernel(plan, sizes_in, sizes_out, count, scalars, *refs):
    n = plan.parts
    ins = [refs[k * len(sizes_in) : (k + 1) * len(sizes_in)] for k in range(n)]
    refs = refs[n * len(sizes_in) :]
    screen_ref, tf_ref, tb_ref, after_ref, *refs = refs
    outs = [refs[k * len(sizes_out) : (k + 1) * len(sizes_out)] for k in range(n)]
    length = plan.length
    for pair in range(plan.rows // 2):
        for solve in range(count):
            columns = []
            for i in range(2):
                row = pair * 2 + i
                parts = []
                for k in range(n):
                    for ref, size in zip(ins[k], sizes_in):
                        first = (solve * plan.rows + row) * size
                        parts.append(ref[first : first + size, :])
                columns.append(jnp.concatenate(parts, axis=0))
            spectrum = along_rows(tf_ref[0], jnp.concatenate(columns, axis=1))
            screen = jnp.concatenate(
                [
                    screen_ref[(pair * 2 + i) * length : (pair * 2 + i + 1) * length, :]
                    for i in range(2)
                ],
                axis=1,
            )
            back = along_rows(tb_ref[0], spectrum * screen)
            for i in range(2):
                row = pair * 2 + i
                for k in range(n):
                    at = k * plan.planes
                    for ref, size in zip(outs[k], sizes_out):
                        first = (solve * plan.rows + row) * size
                        ref[first : first + size, :] = back[
                            at : at + size, i * LANES : (i + 1) * LANES
                        ]
                        at += size


def backward_pair_kernel(plan, scalars, *refs):
    n = plan.parts
    ins, refs = refs[:n], refs[n:]
    p_ref, q_ref, r_ref, tz_ref, ty_ref, _, total_ref, y_ref, z_ref = refs
    even = scalars[1] == 1
    tz, ty = tz_ref[...], ty_ref[0]
    visit = pack_chunk(load_potential(plan, ins, 0, CHUNK, 0, tz, ty), plan)
    mixed = pack_chunk(load_potential(plan, ins, plan.rows * CHUNK, CHUNK, 0, tz, ty), plan)
    p, r = p_ref[...], r_ref[...]
    other = mixed * q_ref[...]
    zero = jnp.zeros_like(other)
    y_ref[...] = mixed * jnp.where(even, r, p)
    z_ref[...] = visit * p + jnp.where(even, other, zero)
    total_ref[...] = visit * r + jnp.where(even, zero, other)


def store_result(out_ref, first, value, plan):
    for i in range(CHUNK):
        wide = unpack(value[i * plan.packed : (i + 1) * plan.packed], plan)
        out_ref[first + i] = wide[:, : plan.breadth]


def backward_own_kernel(plan, scalars, *refs):
    n = plan.parts
    ins, refs = refs[:n], refs[n:]
    chunks = plan.planes // CHUNK
    totals, refs = refs[:chunks], refs[chunks:]
    owns, refs = refs[:chunks], refs[chunks:]
    returned, refs = refs[: 2 * (chunks - 1)], refs[2 * (chunks - 1) :]
    tz_ref, ty_ref, _, out_ref, rest_ref = refs
    for c in range(chunks):
        value = load_potential(plan, ins, 0, plan.planes, c * CHUNK, tz_ref[...], ty_ref[0])
        value = pack_chunk(value, plan) * owns[c][...] + totals[c][...]
        if c < chunks - 1:
            value = value + returned[2 * c][...] + returned[2 * c + 1][...]
            store_result(out_ref, c * CHUNK, value, plan)
        else:
            rest_ref[...] = value


def final_kernel(plan, scalars, partial_ref, rest_ref, y_ref, z_ref, out_ref):
    store_result(out_ref, 0, rest_ref[...] + y_ref[...] + z_ref[...], plan)


def call(kernel, scalars, operands, outs, selected=(), chunk=None, after=None, update=None):
    specs = []
    for operand in operands:
        if any(operand is s for s in selected):
            specs.append(pl.BlockSpec((1,) + operand.shape[1:], lambda i, s: (s[0], 0, 0)))
        elif chunk is not None and operand is chunk[0]:
            specs.append(
                pl.BlockSpec(
                    (CHUNK,) + operand.shape[1:], lambda i, s, c=chunk[1]: (c, 0, 0)
                )
            )
        else:
            zeros = (0,) * operand.ndim
            specs.append(pl.BlockSpec(operand.shape, lambda i, s, zeros=zeros: zeros))
    if after is not None:
        operands = (*operands, after)
        specs.append(pl.BlockSpec(memory_space=pl.ANY))
    out_specs = [pl.BlockSpec(o, lambda i, s, zeros=(0,) * len(o): zeros) for o in outs]
    aliases = {}
    if update is not None:
        specs[0] = pl.BlockSpec(memory_space=pl.ANY)
        out_specs = [
            pl.BlockSpec((CHUNK,) + o[1:], lambda i, s, c=update: (c, 0, 0)) for o in outs
        ]
        aliases = {1: 0}
    return pl.pallas_call(
        kernel,
        grid_spec=pltpu.PrefetchScalarGridSpec(
            num_scalar_prefetch=1,
            grid=(1,),
            in_specs=specs,
            out_specs=out_specs,
        ),
        input_output_aliases=aliases,
        out_shape=[jax.ShapeDtypeStruct(o, F32) for o in outs],
        compiler_params=pltpu.CompilerParams(vmem_limit_bytes=48 * 1024 * 1024),
    )(scalars, *operands)


def exchange(blocks, parts):
    return [blocks[0]] + [
        lax.ppermute(blocks[k], "grid", [(i, i ^ k) for i in range(parts)])
        for k in range(1, parts)
    ]


def exchange_term(bands):
    parts = lax.axis_size("grid")
    number = lax.axis_size("band")
    own = bands[0]
    plan = Plan(*own.shape, parts)
    part = lax.axis_index("grid")
    even = 1 - lax.axis_index("band") % 2
    scalars = jnp.stack([part, even]).astype(jnp.int32)
    swap = [(i, i ^ 1) for i in range(number)]
    behind = [(i, (i - CYCLE) % number) for i in range(number)]
    ahead = [(i, (i + CYCLE) % number) for i in range(number)]
    tz = jnp.asarray(plan.table_z())
    ty_forward, ty_backward = (jnp.asarray(t) for t in plan.table_y())
    tx_forward, tx_backward = (jnp.asarray(t) for t in plan.table_x())
    across, within = (jnp.asarray(t) for t in plan.waves())
    chunks = plan.planes // CHUNK
    whole = own.shape
    packed = (CHUNK * plan.packed, LANES)
    sizes = (plan.planes,)

    (first,) = call(functools.partial(pack_kernel, plan), scalars, (own,), [packed], chunk=(own, 0))
    q, r = [], []

    def shift(chunk):
        q.append(lax.ppermute(chunk, "band", swap))
        r.append(lax.ppermute(chunk, "band", behind))

    shift(first)
    out = call(
        functools.partial(forward_own_kernel, plan),
        scalars,
        (own, tz, ty_forward),
        [(plan.block, LANES)] * parts + [packed] * (chunks - 1),
        (ty_forward,),
        after=first,
    )
    blocks, mine = out[:parts], [first, *out[parts:]]
    own_in = exchange(blocks, parts)
    for c in range(1, chunks):
        shift(mine[c])
    (screen,) = call(
        functools.partial(screen_kernel, plan),
        scalars,
        (across, within),
        [(plan.rows * plan.length, LANES)],
        (within,),
        after=blocks[0],
    )
    after = screen
    pair_in = []
    for c in range(chunks):
        out = call(
            functools.partial(forward_pair_kernel, plan),
            scalars,
            (mine[c], q[c], r[c], tz, ty_forward),
            [(2 * plan.rows * CHUNK, LANES)] * parts,
            (ty_forward,),
            after=after,
        )
        after = out[0]
        pair_in.append(exchange(out, parts))

    def middle(ins, sizes_in, sizes_out, count, after):
        out = call(
            functools.partial(middle_kernel, plan, sizes_in, sizes_out, count),
            scalars,
            (*[block for part in ins for block in part], screen, tx_forward, tx_backward),
            [(count * plan.rows * size, LANES) for size in sizes_out] * parts,
            (tx_forward, tx_backward),
            after=after,
        )
        return [out[i :: len(sizes_out)] for i in range(len(sizes_out))]

    own_mid = middle([[b] for b in own_in], (plan.planes,), sizes, 1, after)
    even_chunks = (CHUNK,) * chunks
    pair_mid = middle(
        [[pair_in[c][k] for c in range(chunks)] for k in range(parts)],
        even_chunks,
        even_chunks,
        2,
        own_mid[0][0],
    )
    pair_back = [exchange(blocks, parts) for blocks in pair_mid]
    own_back = exchange(own_mid[0], parts)
    after = pair_mid[0][0]
    totals, from_y, from_z = [], [], []
    for c in range(chunks):
        total, y, z = call(
            functools.partial(backward_pair_kernel, plan),
            scalars,
            (*pair_back[c], mine[c], q[c], r[c], tz, ty_backward),
            [packed] * 3,
            (ty_backward,),
            after=after,
        )
        after = total
        totals.append(total)
        from_z.append(lax.ppermute(z, "band", ahead))
        from_y.append(lax.ppermute(y, "band", swap))
    partial, rest = call(
        functools.partial(backward_own_kernel, plan),
        scalars,
        (
            *own_back,
            *totals,
            *mine,
            *[part[c] for c in range(chunks - 1) for part in (from_y, from_z)],
            tz,
            ty_backward,
        ),
        [whole, packed],
        (ty_backward,),
        after=after,
    )
    (result,) = call(
        functools.partial(final_kernel, plan),
        scalars,
        (partial, rest, from_y[-1], from_z[-1]),
        [whole],
        update=chunks - 1,
    )
    return result[None]


def solution(mesh):
    return jax.shard_map(
        exchange_term,
        mesh=mesh,
        in_specs=(P("band", "grid", None, None),),
        out_specs=P("band", "grid", None, None),
        check_vma=False,
    )
```

```python
import functools

import jax
import jax.numpy as jnp
import numpy as np
from jax import lax
from jax.experimental import pallas as pl
from jax.experimental.pallas import tpu as pltpu
from jax.sharding import PartitionSpec as P


CYCLE = 2
LANES = 128
F32 = jnp.float32
BF16 = jnp.bfloat16


def cas(rows, columns, length):
    phases = (np.asarray(rows)[:, None] * np.asarray(columns)[None, :]) % length
    angles = 2.0 * np.pi * phases / length
    return np.cos(angles) + np.sin(angles)


def halves(table):
    high = np.asarray(table, np.float32).astype(jnp.bfloat16)
    low = (np.asarray(table, np.float64) - np.asarray(high, np.float64)).astype(np.float32)
    return high, low.astype(jnp.bfloat16)


def doubled(high, low):
    return np.concatenate(
        [np.concatenate([high, high], axis=1), np.concatenate([low, np.zeros_like(low)], axis=1)],
        axis=0,
    )


def wavenumber_sq(indices, length):
    folded = np.minimum(indices, length - indices).astype(np.float32)
    scaled = folded * np.float32(2.0 * np.pi / length)
    return scaled * scaled


class Plan:
    def __init__(self, planes, height, breadth, parts):
        self.planes, self.height, self.breadth, self.parts = planes, height, breadth, parts
        self.length = planes * parts
        self.share = height // parts
        third = breadth // 3
        assert third * 4 == LANES and self.share % 4 == 0 and planes % 8 == 0
        self.third = third
        self.extra = self.share // 4
        self.rows = 3 * self.extra
        assert self.extra <= 8
        self.block = self.rows * planes
        self.packed = 3 * height // 4

    def table_z(self):
        high, low = halves(cas(np.arange(self.breadth), np.arange(self.breadth), self.breadth))
        out = np.zeros((2 * LANES, 2 * LANES), jnp.bfloat16)
        n = self.breadth
        out[:n, :n] = high
        out[:n, LANES : LANES + n] = low
        out[LANES : LANES + n, :n] = high
        return out

    def positions(self, part):
        rows, index = [], []
        for k in range(self.parts):
            base = self.share * (part ^ k)
            for t in range(3):
                for q in range(self.extra):
                    rows.append((k * 3 + t) * 8 + q)
                    index.append(base + t * self.extra + q)
            for q in range(self.extra):
                rows.append((self.parts * 3 + k) * 8 + q)
                index.append(base + 3 * self.extra + q)
        return np.array(rows), np.array(index)

    def table_y(self):
        m = self.parts * 32
        forward, backward = [], []
        for part in range(self.parts):
            rows, index = self.positions(part)
            full = np.zeros((m, self.height))
            full[rows] = cas(index, np.arange(self.height), self.height)
            high, low = halves(full)
            forward.append(doubled(high, low))
            backward.append(doubled(high.T, low.T))
        return np.stack(forward), np.stack(backward)

    def table_x(self):
        forward, backward = [], []
        for part in range(self.parts):
            order = np.concatenate(
                [np.arange(self.planes) + self.planes * (part ^ k) for k in range(self.parts)]
            )
            high, low = halves(cas(np.arange(self.length), order, self.length))
            forward.append(doubled(high, low))
            backward.append(doubled(high.T, low.T))
        return np.stack(forward), np.stack(backward)

    def waves(self):
        across = np.broadcast_to(
            wavenumber_sq(np.arange(self.length), self.length)[:, None], (self.length, LANES)
        )
        row = np.arange(self.rows)[:, None]
        lane = np.arange(LANES)[None, :]
        main = lane < self.breadth
        y = np.where(main, row, 3 * self.extra + row % self.extra)
        z = np.where(main, lane, self.third * (row // self.extra) + lane - self.breadth)
        within = np.zeros((self.parts, -(-self.rows // 8) * 8, LANES), np.float32)
        for part in range(self.parts):
            within[part, : self.rows] = wavenumber_sq(
                part * self.share + y, self.height
            ) + wavenumber_sq(z, self.breadth)
        return np.array(across), within


def split(value):
    high = value.astype(BF16)
    return high, (value - high.astype(F32)).astype(BF16)


def dot(a, b):
    return jnp.dot(a, b, preferred_element_type=F32)


def lanes(shape):
    return lax.broadcasted_iota(jnp.int32, shape, len(shape) - 1)


def along_rows(table, value):
    both = dot(table, jnp.concatenate(split(value), axis=0))
    half = both.shape[0] // 2
    return both[:half] + both[half:]


def along_lanes(value, table):
    both = dot(jnp.concatenate(split(value), axis=1), table)
    return both[:, :LANES] + both[:, LANES:]


def widen(value):
    rows, width = value.shape
    return jnp.concatenate([value, jnp.zeros((rows, LANES - width), value.dtype)], axis=1)


def pack(wide, plan):
    h = plan.height // 4
    tail = wide[3 * h :]
    parts = []
    for t in range(3):
        main = wide[t * h : (t + 1) * h]
        moved = pltpu.roll(tail, plan.breadth - plan.third * t, 1)
        parts.append(jnp.where(lanes(main.shape) < plan.breadth, main, moved))
    return jnp.concatenate(parts, axis=0)


def thirds(parts, plan):
    tail = None
    for t, part in enumerate(parts):
        moved = pltpu.roll(part, (plan.third * (t + 1)) % LANES, 1)
        tail = moved if tail is None else jnp.where(lanes(part.shape) < plan.third * t, tail, moved)
    return tail


def unpack(value, plan):
    h = plan.height // 4
    return jnp.concatenate(
        [value, thirds([value[t * h : (t + 1) * h] for t in range(3)], plan)], axis=0
    )


def store_spectrum(plan, density, tz, ty, outs, base, stride, plane):
    h, e = plan.height, plan.extra
    once = along_lanes(density, tz)
    for pair in range(CHUNK // 2):
        two = jnp.concatenate(
            [once[(2 * pair + i) * h : (2 * pair + i + 1) * h] for i in range(2)], axis=1
        )
        spectrum = along_rows(ty, two)
        for i in range(2):
            s = spectrum[:, i * LANES : (i + 1) * LANES]
            for k in range(plan.parts):
                tail = s[(3 * plan.parts + k) * 8 : (3 * plan.parts + k + 1) * 8]
                for t in range(3):
                    main = s[(k * 3 + t) * 8 : (k * 3 + t + 1) * 8]
                    moved = pltpu.roll(tail, plan.breadth - plan.third * t, 1)
                    packed = jnp.where(lanes(main.shape) < plan.breadth, main, moved)
                    first = base + t * e * stride + plane + 2 * pair + i
                    outs[k][pl.ds(first, e, stride=stride), :] = packed[:e]


def load_potential(plan, place, planes, tz, ty):
    e = plan.extra
    found = []
    for first in range(0, len(planes), 2):
        two = []
        for plane in planes[first : first + 2]:
            ins, stride, offset = place(plane)
            rows, tails = [], []
            for ref, base in ins:
                parts = []
                for t in range(3):
                    at = base + t * e * stride + offset
                    part = ref[pl.ds(at, e, stride=stride), :]
                    parts.append(jnp.concatenate([part, jnp.zeros((8 - e, LANES), F32)], axis=0))
                rows += parts
                tails.append(thirds(parts, plan))
            two.append(jnp.concatenate(rows + tails, axis=0))
        once = along_rows(ty, jnp.concatenate(two, axis=1))
        found += [once[:, :LANES], once[:, LANES:]]
    return along_lanes(jnp.concatenate(found, axis=0), tz)


CHUNK = 8


def pack_kernel(plan, scalars, own_ref, out):
    for i in range(CHUNK):
        out[i * plan.packed : (i + 1) * plan.packed, :] = pack(widen(own_ref[i]), plan)


def unpack_chunk(value, plan):
    return jnp.concatenate(
        [unpack(value[i * plan.packed : (i + 1) * plan.packed], plan) for i in range(CHUNK)],
        axis=0,
    )


def pack_chunk(wide, plan):
    h = plan.height
    return jnp.concatenate(
        [pack(wide[i * h : (i + 1) * h], plan) for i in range(wide.shape[0] // h)], axis=0
    )


def planes_of(refs, first, size, plan):
    parts = []
    while size:
        c, at = divmod(first, CHUNK)
        count = min(size, CHUNK - at)
        parts.append(refs[c][at * plan.packed : (at + count) * plan.packed, :])
        first, size = first + count, size - count
    return jnp.concatenate(parts, axis=0)


def forward_own_kernel(plan, scalars, own_ref, tz_ref, ty_ref, after_ref, *outs):
    blocks, later = outs[: plan.parts], outs[plan.parts :]
    for c in range(plan.planes // CHUNK):
        here = slice(c * CHUNK, (c + 1) * CHUNK)
        wide = widen(own_ref[here].reshape(CHUNK * plan.height, plan.breadth))
        if c:
            later[c - 1][...] = pack_chunk(wide, plan)
        store_spectrum(
            plan, wide * wide, tz_ref[...], ty_ref[0], blocks, 0, plan.planes, c * CHUNK
        )


def forward_pair_kernel(plan, scalars, p_ref, q_ref, r_ref, tz_ref, ty_ref, after_ref, *outs):
    even = scalars[1] == 1
    p, r = p_ref[...], r_ref[...]
    tz, ty = tz_ref[...], ty_ref[0]
    store_spectrum(plan, unpack_chunk(p * r, plan), tz, ty, outs, 0, CHUNK, 0)
    mixed = q_ref[...] * jnp.where(even, r, p)
    store_spectrum(plan, unpack_chunk(mixed, plan), tz, ty, outs, plan.rows * CHUNK, CHUNK, 0)


def screen_kernel(plan, scalars, across_ref, within_ref, after_ref, out_ref):
    cells = plan.length * plan.height * plan.breadth
    limit = 4.0 * np.pi / plan.length
    rate = 1.0 / (4.0 * limit * limit)
    for row in range(plan.rows):
        wave_sq = across_ref[...] + within_ref[0, row : row + 1, :]
        guarded = jnp.where(wave_sq > 0, wave_sq, 1.0)
        screened = (-0.2 * 4.0 * np.pi / cells) / guarded * (1.0 - jnp.exp(guarded * -rate))
        out_ref[row * plan.length : (row + 1) * plan.length, :] = jnp.where(
            wave_sq > 0, screened, 0.0
        )


JOINED = 2


def places(refs, plan, sizes, count):
    joined, cut = refs[:JOINED], refs[JOINED:]
    result, row = [], 0
    for i, size in enumerate(sizes):
        result.append([(ref, row) for ref in joined] + [(ref, 0) for ref in cut[i :: len(sizes)]])
        row += count * plan.rows * size
    return result


def shapes_of(plan, sizes, count):
    rows = [count * plan.rows * size for size in sizes]
    return [(sum(rows), LANES)] * JOINED + [(n, LANES) for n in rows] * (plan.parts - JOINED)


def middle_kernel(plan, sizes_in, sizes_out, count, scalars, *refs):
    n = plan.parts
    ins = [refs[k * len(sizes_in) : (k + 1) * len(sizes_in)] for k in range(n)]
    refs = refs[n * len(sizes_in) :]
    screen_ref, tf_ref, tb_ref, after_ref, *refs = refs
    outs = places(refs, plan, sizes_out, count)
    length = plan.length
    for pair in range(plan.rows // 2):
        for solve in range(count):
            columns = []
            for i in range(2):
                row = pair * 2 + i
                parts = []
                for k in range(n):
                    for ref, size in zip(ins[k], sizes_in):
                        first = (solve * plan.rows + row) * size
                        parts.append(ref[first : first + size, :])
                columns.append(jnp.concatenate(parts, axis=0))
            spectrum = along_rows(tf_ref[0], jnp.concatenate(columns, axis=1))
            screen = jnp.concatenate(
                [
                    screen_ref[(pair * 2 + i) * length : (pair * 2 + i + 1) * length, :]
                    for i in range(2)
                ],
                axis=1,
            )
            back = along_rows(tb_ref[0], spectrum * screen)
            for i in range(2):
                row = pair * 2 + i
                at = 0
                for out, size in zip(outs, sizes_out):
                    for k, (ref, base) in enumerate(out):
                        first = base + (solve * plan.rows + row) * size
                        ref[first : first + size, :] = back[
                            k * plan.planes + at : k * plan.planes + at + size,
                            i * LANES : (i + 1) * LANES,
                        ]
                    at += size


def backward_pair_kernel(plan, pieces, piece, scalars, *refs):
    n = plan.parts
    ins, refs = refs[:n], refs[n:]
    first, size = sum(pieces[:piece]), pieces[piece]
    skipped = 2 * plan.rows * first
    chunks = plan.planes // CHUNK
    fields = [planes_of(refs[i * chunks : (i + 1) * chunks], first, size, plan) for i in range(3)]
    tz_ref, ty_ref, _, total_ref, y_ref, z_ref = refs[3 * chunks :]
    even = scalars[1] == 1
    tz, ty = tz_ref[...], ty_ref[0]

    def solved(which):
        base = which * plan.rows * size
        found = [(ref, base + (skipped if k < JOINED else 0)) for k, ref in enumerate(ins)]
        wide = load_potential(plan, lambda i: (found, size, i), range(size), tz, ty)
        return pack_chunk(wide, plan)

    visit, mixed = solved(0), solved(1)
    p, q, r = fields
    other = mixed * q
    zero = jnp.zeros_like(other)
    y_ref[...] = mixed * jnp.where(even, r, p)
    z_ref[...] = visit * p + jnp.where(even, other, zero)
    total_ref[...] = visit * r + jnp.where(even, zero, other)


def store_result(out_ref, first, value, plan):
    for i in range(value.shape[0] // plan.packed):
        wide = unpack(value[i * plan.packed : (i + 1) * plan.packed], plan)
        out_ref[first + i] = wide[:, : plan.breadth]


LATE = 1


def backward_own_kernel(plan, sizes, pieces, scalars, *refs):
    used = JOINED + (plan.parts - JOINED) * len(sizes)
    ins, refs = places(refs[:used], plan, sizes, 1), refs[used:]
    count, chunks = len(pieces), plan.planes // CHUNK
    ready = count - LATE
    totals, refs = refs[:count], refs[count:]
    owns, refs = refs[:chunks], refs[chunks:]
    returned, refs = refs[: 2 * ready], refs[2 * ready :]
    tz_ref, ty_ref, after_ref, out_ref, *rest = refs

    def place(plane):
        which = 0
        while plane >= sizes[which]:
            plane -= sizes[which]
            which += 1
        return ins[which], sizes[which], plane

    first = 0
    for c, size in enumerate(pieces):
        value = load_potential(plan, place, range(first, first + size), tz_ref[...], ty_ref[0])
        value = pack_chunk(value, plan) * planes_of(owns, first, size, plan) + totals[c][...]
        if c < ready:
            value = value + returned[2 * c][...] + returned[2 * c + 1][...]
            store_result(out_ref, first, value, plan)
        else:
            rest[c - ready][...] = value
        first += size


def final_kernel(plan, scalars, partial_ref, *refs):
    rest, ys, zs, out_ref = refs[:LATE], refs[LATE : 2 * LATE], refs[2 * LATE : 3 * LATE], refs[-1]
    first = 0
    for part, y, z in zip(rest, ys, zs):
        store_result(out_ref, first, part[...] + y[...] + z[...], plan)
        first += part.shape[0] // plan.packed


def call(kernel, scalars, operands, outs, selected=(), chunk=None, after=None, update=None):
    specs = []
    for operand in operands:
        if any(operand is s for s in selected):
            specs.append(pl.BlockSpec((1,) + operand.shape[1:], lambda i, s: (s[0], 0, 0)))
        elif chunk is not None and operand is chunk[0]:
            specs.append(
                pl.BlockSpec(
                    (CHUNK,) + operand.shape[1:], lambda i, s, c=chunk[1]: (c, 0, 0)
                )
            )
        else:
            zeros = (0,) * operand.ndim
            specs.append(pl.BlockSpec(operand.shape, lambda i, s, zeros=zeros: zeros))
    if after is not None:
        operands = (*operands, after)
        specs.append(pl.BlockSpec(memory_space=pl.ANY))
    out_specs = [pl.BlockSpec(o, lambda i, s, zeros=(0,) * len(o): zeros) for o in outs]
    aliases = {}
    if update is not None:
        specs[0] = pl.BlockSpec(memory_space=pl.ANY)
        out_specs = [
            pl.BlockSpec((update,) + o[1:], lambda i, s, c=o[0] // update - 1: (c, 0, 0))
            for o in outs
        ]
        aliases = {1: 0}
    return pl.pallas_call(
        kernel,
        grid_spec=pltpu.PrefetchScalarGridSpec(
            num_scalar_prefetch=1,
            grid=(1,),
            in_specs=specs,
            out_specs=out_specs,
        ),
        input_output_aliases=aliases,
        out_shape=[jax.ShapeDtypeStruct(o, F32) for o in outs],
        compiler_params=pltpu.CompilerParams(vmem_limit_bytes=48 * 1024 * 1024),
    )(scalars, *operands)


def send(block, k, parts):
    return lax.ppermute(block, "grid", [(i, i ^ k) for i in range(parts)])


def exchange(blocks, parts):
    far = [send(blocks[k], k, parts) for k in range(2, parts)]
    return [blocks[0], send(blocks[1], 1, parts), *far]


def exchange_pieces(blocks, parts, count):
    near = send(blocks[1], 1, parts)
    far = [send(block, JOINED + i // count, parts) for i, block in enumerate(blocks[JOINED:])]
    return [blocks[0], near, *far]


PIECES = 3


def pieces_of(planes):
    return (planes // PIECES,) * PIECES


def exchange_term(bands):
    parts = lax.axis_size("grid")
    number = lax.axis_size("band")
    own = bands[0]
    plan = Plan(*own.shape, parts)
    part = lax.axis_index("grid")
    even = lax.axis_index("band") % 2
    scalars = jnp.stack([part, even]).astype(jnp.int32)
    swap = [(i, i ^ 1) for i in range(number)]
    behind = [(i, (i + CYCLE) % number) for i in range(number)]
    ahead = [(i, (i - CYCLE) % number) for i in range(number)]
    tz = jnp.asarray(plan.table_z())
    ty_forward, ty_backward = (jnp.asarray(t) for t in plan.table_y())
    tx_forward, tx_backward = (jnp.asarray(t) for t in plan.table_x())
    across, within = (jnp.asarray(t) for t in plan.waves())
    chunks = plan.planes // CHUNK
    whole = own.shape
    packed = (CHUNK * plan.packed, LANES)
    sizes = (CHUNK, plan.planes - CHUNK)
    pieces = pieces_of(plan.planes)

    (first,) = call(functools.partial(pack_kernel, plan), scalars, (own,), [packed], chunk=(own, 0))
    q, r = [], []

    def shift(chunk):
        q.append(lax.ppermute(chunk, "band", swap))
        r.append(lax.ppermute(chunk, "band", behind))

    shift(first)
    out = call(
        functools.partial(forward_own_kernel, plan),
        scalars,
        (own, tz, ty_forward),
        [(plan.block, LANES)] * parts + [packed] * (chunks - 1),
        (ty_forward,),
        after=first,
    )
    blocks, mine = out[:parts], [first, *out[parts:]]
    own_in = exchange(blocks, parts)
    for c in range(1, chunks):
        shift(mine[c])
    after = blocks[0]
    pair_in = []
    for c in range(chunks):
        out = call(
            functools.partial(forward_pair_kernel, plan),
            scalars,
            (mine[c], q[c], r[c], tz, ty_forward),
            [(2 * plan.rows * CHUNK, LANES)] * parts,
            (ty_forward,),
            after=after,
        )
        after = out[0]
        pair_in.append(exchange(out, parts))
    (screen,) = call(
        functools.partial(screen_kernel, plan),
        scalars,
        (across, within),
        [(plan.rows * plan.length, LANES)],
        (within,),
        after=after,
    )

    def middle(ins, sizes_in, sizes_out, count, after):
        return call(
            functools.partial(middle_kernel, plan, sizes_in, sizes_out, count),
            scalars,
            (*[block for part in ins for block in part], screen, tx_forward, tx_backward),
            shapes_of(plan, sizes_out, count),
            (tx_forward, tx_backward),
            after=after,
        )

    own_mid = middle([[b] for b in own_in], (plan.planes,), sizes, 1, screen)
    own_back = exchange_pieces(own_mid, parts, len(sizes))
    pair_mid = middle(
        [[pair_in[c][k] for c in range(chunks)] for k in range(parts)],
        (CHUNK,) * chunks,
        pieces,
        2,
        own_mid[0],
    )
    pair_back = exchange_pieces(pair_mid, parts, len(pieces))
    after = pair_mid[0]
    totals, from_y, from_z = [], [], []
    for c, size in enumerate(pieces):
        piece = (size * plan.packed, LANES)
        total, y, z = call(
            functools.partial(backward_pair_kernel, plan, pieces, c),
            scalars,
            (
                *pair_back[:JOINED],
                *pair_back[JOINED + c :: len(pieces)],
                *mine,
                *q,
                *r,
                tz,
                ty_backward,
            ),
            [piece] * 3,
            (ty_backward,),
            after=after,
        )
        after = total
        totals.append(total)
        from_z.append(lax.ppermute(z, "band", ahead))
        from_y.append(lax.ppermute(y, "band", swap))
    ready = len(pieces) - LATE
    partial, *rest = call(
        functools.partial(backward_own_kernel, plan, sizes, pieces),
        scalars,
        (
            *own_back,
            *totals,
            *mine,
            *[part[c] for c in range(ready) for part in (from_y, from_z)],
            tz,
            ty_backward,
        ),
        [whole] + [(size * plan.packed, LANES) for size in pieces[ready:]],
        (ty_backward,),
        after=after,
    )
    (result,) = call(
        functools.partial(final_kernel, plan),
        scalars,
        (partial, *rest, *from_y[ready:], *from_z[ready:]),
        [whole],
        update=sum(pieces[ready:]),
    )
    return result[None]


def solution(mesh):
    return jax.shard_map(
        exchange_term,
        mesh=mesh,
        in_specs=(P("band", "grid", None, None),),
        out_specs=P("band", "grid", None, None),
        check_vma=False,
    )
```

```python
import functools
from typing import NamedTuple

import jax
import jax.numpy as jnp
import numpy as np
from jax import lax
from jax.experimental import pallas as pl
from jax.experimental.pallas import tpu as pltpu
from jax.sharding import PartitionSpec as P


CYCLE = 2
LANES = 128
F32 = jnp.float32
BF16 = jnp.bfloat16


def cas(rows, columns, length):
    phases = (np.asarray(rows)[:, None] * np.asarray(columns)[None, :]) % length
    angles = 2.0 * np.pi * phases / length
    return np.cos(angles) + np.sin(angles)


def halves(table):
    high = np.asarray(table, np.float32).astype(jnp.bfloat16)
    low = (np.asarray(table, np.float64) - np.asarray(high, np.float64)).astype(np.float32)
    return high, low.astype(jnp.bfloat16)


def doubled(high, low):
    return np.concatenate(
        [np.concatenate([high, high], axis=1), np.concatenate([low, np.zeros_like(low)], axis=1)],
        axis=0,
    )


def wavenumber_sq(indices, length):
    folded = np.minimum(indices, length - indices).astype(np.float32)
    scaled = folded * np.float32(2.0 * np.pi / length)
    return scaled * scaled


class Plan:
    def __init__(self, planes, height, breadth, parts):
        self.planes, self.height, self.breadth, self.parts = planes, height, breadth, parts
        self.length = planes * parts
        self.share = height // parts
        third = breadth // 3
        assert third * 4 == LANES and self.share % 4 == 0 and planes % 8 == 0
        self.third = third
        self.extra = self.share // 4
        self.rows = 3 * self.extra
        assert self.extra <= 8
        self.block = self.rows * planes
        self.packed = 3 * height // 4

    def table_z(self):
        high, low = halves(cas(np.arange(self.breadth), np.arange(self.breadth), self.breadth))
        out = np.zeros((2 * LANES, 2 * LANES), jnp.bfloat16)
        n = self.breadth
        out[:n, :n] = high
        out[:n, LANES : LANES + n] = low
        out[LANES : LANES + n, :n] = high
        return out

    def positions(self, part):
        rows, index = [], []
        for k in range(self.parts):
            base = self.share * (part ^ k)
            for t in range(3):
                for q in range(self.extra):
                    rows.append((k * 3 + t) * 8 + q)
                    index.append(base + t * self.extra + q)
            for q in range(self.extra):
                rows.append((self.parts * 3 + k) * 8 + q)
                index.append(base + 3 * self.extra + q)
        return np.array(rows), np.array(index)

    def table_y(self):
        m = self.parts * 32
        forward, backward = [], []
        for part in range(self.parts):
            rows, index = self.positions(part)
            full = np.zeros((m, self.height))
            full[rows] = cas(index, np.arange(self.height), self.height)
            high, low = halves(full)
            forward.append(doubled(high, low))
            backward.append(doubled(high.T, low.T))
        return np.stack(forward), np.stack(backward)

    def table_x(self):
        forward, backward = [], []
        for part in range(self.parts):
            order = np.concatenate(
                [np.arange(self.planes) + self.planes * (part ^ k) for k in range(self.parts)]
            )
            high, low = halves(cas(np.arange(self.length), order, self.length))
            forward.append(doubled(high, low))
            backward.append(doubled(high.T, low.T))
        return np.stack(forward), np.stack(backward)

    def waves(self):
        across = np.broadcast_to(
            wavenumber_sq(np.arange(self.length), self.length)[:, None], (self.length, LANES)
        )
        row = np.arange(self.rows)[:, None]
        lane = np.arange(LANES)[None, :]
        main = lane < self.breadth
        y = np.where(main, row, 3 * self.extra + row % self.extra)
        z = np.where(main, lane, self.third * (row // self.extra) + lane - self.breadth)
        within = np.zeros((self.parts, -(-self.rows // 8) * 8, LANES), np.float32)
        for part in range(self.parts):
            within[part, : self.rows] = wavenumber_sq(
                part * self.share + y, self.height
            ) + wavenumber_sq(z, self.breadth)
        return np.array(across), within


def split(value):
    high = value.astype(BF16)
    return high, (value - high.astype(F32)).astype(BF16)


def dot(a, b):
    return jnp.dot(a, b, preferred_element_type=F32)


def lanes(shape):
    return lax.broadcasted_iota(jnp.int32, shape, len(shape) - 1)


def along_rows(table, value):
    both = dot(table, jnp.concatenate(split(value), axis=0))
    half = both.shape[0] // 2
    return both[:half] + both[half:]


def along_lanes(value, table):
    both = dot(jnp.concatenate(split(value), axis=1), table)
    return both[:, :LANES] + both[:, LANES:]


def widen(value):
    rows, width = value.shape
    return jnp.concatenate([value, jnp.zeros((rows, LANES - width), value.dtype)], axis=1)


def pack(wide, plan):
    h = plan.height // 4
    tail = wide[3 * h :]
    parts = []
    for t in range(3):
        main = wide[t * h : (t + 1) * h]
        moved = pltpu.roll(tail, plan.breadth - plan.third * t, 1)
        parts.append(jnp.where(lanes(main.shape) < plan.breadth, main, moved))
    return jnp.concatenate(parts, axis=0)


def thirds(parts, plan):
    tail = None
    for t, part in enumerate(parts):
        moved = pltpu.roll(part, (plan.third * (t + 1)) % LANES, 1)
        tail = moved if tail is None else jnp.where(lanes(part.shape) < plan.third * t, tail, moved)
    return tail


def unpack(value, plan):
    h = plan.height // 4
    return jnp.concatenate(
        [value, thirds([value[t * h : (t + 1) * h] for t in range(3)], plan)], axis=0
    )


def store_spectrum(plan, density, tz, ty, outs, base, stride, plane):
    h, e = plan.height, plan.extra
    once = along_lanes(density, tz)
    for pair in range(CHUNK // 2):
        two = jnp.concatenate(
            [once[(2 * pair + i) * h : (2 * pair + i + 1) * h] for i in range(2)], axis=1
        )
        spectrum = along_rows(ty, two)
        for i in range(2):
            s = spectrum[:, i * LANES : (i + 1) * LANES]
            for k in range(plan.parts):
                tail = s[(3 * plan.parts + k) * 8 : (3 * plan.parts + k + 1) * 8]
                for t in range(3):
                    main = s[(k * 3 + t) * 8 : (k * 3 + t + 1) * 8]
                    moved = pltpu.roll(tail, plan.breadth - plan.third * t, 1)
                    packed = jnp.where(lanes(main.shape) < plan.breadth, main, moved)
                    first = base + t * e * stride + plane + 2 * pair + i
                    outs[k][pl.ds(first, e, stride=stride), :] = packed[:e]


def load_potential(plan, place, planes, tz, ty):
    e = plan.extra
    found = []
    for first in range(0, len(planes), 2):
        two = []
        for plane in planes[first : first + 2]:
            rows, tails = [], []
            for ref, stride, offset in place(plane):
                parts = []
                for t in range(3):
                    at = t * e * stride + offset
                    part = ref[pl.ds(at, e, stride=stride), :]
                    parts.append(jnp.concatenate([part, jnp.zeros((8 - e, LANES), F32)], axis=0))
                rows += parts
                tails.append(thirds(parts, plan))
            two.append(jnp.concatenate(rows + tails, axis=0))
        once = along_rows(ty, jnp.concatenate(two, axis=1))
        found += [once[:, :LANES], once[:, LANES:]]
    return along_lanes(jnp.concatenate(found, axis=0), tz)


CHUNK = 8
PIECES = 3
LATE = 1


def pack_kernel(plan, scalars, ins, outs):
    for i in range(CHUNK):
        outs[0][i * plan.packed : (i + 1) * plan.packed, :] = pack(widen(ins[0][i]), plan)


def unpack_chunk(value, plan):
    return jnp.concatenate(
        [unpack(value[i * plan.packed : (i + 1) * plan.packed], plan) for i in range(CHUNK)],
        axis=0,
    )


def pack_chunk(wide, plan):
    h = plan.height
    return jnp.concatenate(
        [pack(wide[i * h : (i + 1) * h], plan) for i in range(wide.shape[0] // h)], axis=0
    )


def planes_of(refs, first, size, plan):
    parts = []
    while size:
        c, at = divmod(first, CHUNK)
        count = min(size, CHUNK - at)
        parts.append(refs[c][at * plan.packed : (at + count) * plan.packed, :])
        first, size = first + count, size - count
    return jnp.concatenate(parts, axis=0)


def forward_own_kernel(plan, scalars, ins, outs):
    own_ref, tz_ref, ty_ref = ins
    blocks, later = outs[: plan.parts], outs[plan.parts :]
    for c in range(plan.planes // CHUNK):
        here = slice(c * CHUNK, (c + 1) * CHUNK)
        wide = widen(own_ref[here].reshape(CHUNK * plan.height, plan.breadth))
        if c:
            later[c - 1][...] = pack_chunk(wide, plan)
        store_spectrum(
            plan, wide * wide, tz_ref[...], ty_ref[0], blocks, 0, plan.planes, c * CHUNK
        )


def forward_pair_kernel(plan, scalars, ins, outs):
    p_ref, q_ref, r_ref, tz_ref, ty_ref = ins
    even = scalars[1] == 1
    p, r = p_ref[...], r_ref[...]
    tz, ty = tz_ref[...], ty_ref[0]
    apart = len(outs) > plan.parts
    blocks, base = (outs[plan.parts :], 0) if apart else (outs, plan.rows * CHUNK)
    mixed = q_ref[...] * jnp.where(even, r, p)
    store_spectrum(plan, unpack_chunk(mixed, plan), tz, ty, blocks, base, CHUNK, 0)
    store_spectrum(plan, unpack_chunk(p * r, plan), tz, ty, outs[: plan.parts], 0, CHUNK, 0)


def screen_kernel(plan, scalars, ins, outs):
    across_ref, within_ref = ins
    cells = plan.length * plan.height * plan.breadth
    limit = 4.0 * np.pi / plan.length
    rate = 1.0 / (4.0 * limit * limit)
    for row in range(plan.rows):
        wave_sq = across_ref[...] + within_ref[0, row : row + 1, :]
        guarded = jnp.where(wave_sq > 0, wave_sq, 1.0)
        screened = (-0.2 * 4.0 * np.pi / cells) / guarded * (1.0 - jnp.exp(guarded * -rate))
        outs[0][row * plan.length : (row + 1) * plan.length, :] = jnp.where(
            wave_sq > 0, screened, 0.0
        )


def middle_kernel(plan, chunks, sizes, scalars, ins, outs):
    n, length = plan.parts, plan.length
    blocks = [ins[k * len(chunks) : (k + 1) * len(chunks)] for k in range(n)]
    screen_ref, tf_ref, tb_ref = ins[n * len(chunks) :]
    cut = [outs[2 + i * len(sizes) : 2 + (i + 1) * len(sizes)] for i in range(n - 2)]
    for pair in range(plan.rows // 2):
        columns = []
        for row in (pair * 2, pair * 2 + 1):
            parts = []
            for part in blocks:
                for ref, (size, base) in zip(part, chunks):
                    parts.append(ref[base + row * size : base + (row + 1) * size, :])
            columns.append(jnp.concatenate(parts, axis=0))
        spectrum = along_rows(tf_ref[0], jnp.concatenate(columns, axis=1))
        screen = jnp.concatenate(
            [
                screen_ref[row * length : (row + 1) * length, :]
                for row in (pair * 2, pair * 2 + 1)
            ],
            axis=1,
        )
        back = along_rows(tb_ref[0], spectrum * screen)
        for i in range(2):
            row, lane = pair * 2 + i, slice(i * LANES, (i + 1) * LANES)
            for k in range(n):
                at = k * plan.planes
                refs = cut[k - 2] if k >= 2 else outs[k : k + 1]
                for ref, size in zip(refs, sizes if k >= 2 else (plan.planes,)):
                    ref[row * size : (row + 1) * size, :] = back[at : at + size, lane]
                    at += size


def backward_pair_kernel(plan, pieces, piece, scalars, ins, outs):
    far = plan.parts - 2
    whole, ins = ins[:4], ins[4:]
    apart = piece == 0
    blocks, ins = ins[: far * (1 + apart)], ins[far * (1 + apart) :]
    chunks = plan.planes // CHUNK
    first, size = sum(pieces[:piece]), pieces[piece]
    p, q, r = (
        planes_of(ins[i * chunks : (i + 1) * chunks], first, size, plan) for i in range(3)
    )
    tz, ty = ins[3 * chunks][...], ins[3 * chunks + 1][0]
    even = scalars[1] == 1

    def solved(which):
        base = 0 if apart else which * plan.rows * size
        refs = blocks[which * far : (which + 1) * far] if apart else blocks

        def place(i):
            near = [(ref, plan.planes, first + i) for ref in whole[2 * which : 2 * which + 2]]
            return near + [(ref, size, base + i) for ref in refs]

        return pack_chunk(load_potential(plan, place, range(size), tz, ty), plan)

    mixed, visit = solved(0), solved(1)
    total_ref, y_ref, z_ref = outs
    other = mixed * q
    zero = jnp.zeros_like(other)
    y_ref[...] = mixed * jnp.where(even, r, p)
    z_ref[...] = visit * p + jnp.where(even, other, zero)
    total_ref[...] = visit * r + jnp.where(even, zero, other)


def store_result(out_ref, first, value, plan):
    for i in range(value.shape[0] // plan.packed):
        wide = unpack(value[i * plan.packed : (i + 1) * plan.packed], plan)
        out_ref[first + i] = wide[:, : plan.breadth]


def backward_own_kernel(plan, pieces, scalars, ins, outs):
    n, count, chunks = plan.parts, len(pieces), plan.planes // CHUNK
    ready = count - LATE
    blocks, ins = ins[:n], ins[n:]
    totals, ins = ins[:count], ins[count:]
    owns, ins = ins[:chunks], ins[chunks:]
    returned, (tz_ref, ty_ref) = ins[: 2 * ready], ins[2 * ready :]
    out_ref, *rest = outs

    def place(plane):
        return [(ref, plan.planes, plane) for ref in blocks]

    first = 0
    for c, size in enumerate(pieces):
        value = load_potential(plan, place, range(first, first + size), tz_ref[...], ty_ref[0])
        value = pack_chunk(value, plan) * planes_of(owns, first, size, plan) + totals[c][...]
        if c < ready:
            value = value + returned[2 * c][...] + returned[2 * c + 1][...]
            store_result(out_ref, first, value, plan)
        else:
            rest[c - ready][...] = value
        first += size


def final_kernel(plan, scalars, ins, outs):
    rest, ys, zs = ins[:LATE], ins[LATE : 2 * LATE], ins[2 * LATE :]
    first = 0
    for part, y, z in zip(rest, ys, zs):
        store_result(outs[0], first, part[...] + y[...] + z[...], plan)
        first += part.shape[0] // plan.packed


class Block(NamedTuple):
    shape: tuple
    rows: int
    index: int
    array: jax.Array | None = None


def call(kernel, scalars, operands, outs, selected=(), chunk=None, after=None):
    specs = []
    for operand in operands:
        if any(operand is s for s in selected):
            specs.append(pl.BlockSpec((1,) + operand.shape[1:], lambda i, s: (s[0], 0, 0)))
        elif chunk is not None and operand is chunk[0]:
            specs.append(
                pl.BlockSpec((CHUNK,) + operand.shape[1:], lambda i, s, c=chunk[1]: (c, 0, 0))
            )
        else:
            zeros = (0,) * operand.ndim
            specs.append(pl.BlockSpec(operand.shape, lambda i, s, zeros=zeros: zeros))
    count = len(operands)
    extras = [] if after is None else [after]
    out_specs, shapes, aliases = [], [], {}
    for i, out in enumerate(outs):
        if not isinstance(out, Block):
            out = Block(out, out[0], 0)
        if out.array is not None:
            extras.append(out.array)
            aliases[count + len(extras)] = i
        shapes.append(jax.ShapeDtypeStruct(out.shape, F32))
        at = (out.index,) + (0,) * (len(out.shape) - 1)
        out_specs.append(pl.BlockSpec((out.rows,) + out.shape[1:], lambda i, s, at=at: at))
    seen = count + len(extras)

    def body(scalars, *refs):
        kernel(scalars, refs[:count], refs[seen:])

    return pl.pallas_call(
        body,
        grid_spec=pltpu.PrefetchScalarGridSpec(
            num_scalar_prefetch=1,
            grid=(1,),
            in_specs=specs + [pl.BlockSpec(memory_space=pl.ANY)] * len(extras),
            out_specs=out_specs,
        ),
        input_output_aliases=aliases,
        out_shape=shapes,
        compiler_params=pltpu.CompilerParams(vmem_limit_bytes=48 * 1024 * 1024),
    )(scalars, *operands, *extras)


def send(block, k, parts):
    return lax.ppermute(block, "grid", [(i, i ^ k) for i in range(parts)])


def send_far(blocks, parts):
    return [send(block, k, parts) for k, block in zip(range(2, parts), blocks)]


def exchange(blocks, parts):
    far = send_far(blocks[2:], parts)
    return [blocks[0], send(blocks[1], 1, parts), *far]


def pieces_of(planes):
    return (planes // PIECES,) * PIECES


def exchange_term(bands):
    parts = lax.axis_size("grid")
    number = lax.axis_size("band")
    own = bands[0]
    plan = Plan(*own.shape, parts)
    part = lax.axis_index("grid")
    even = lax.axis_index("band") % 2
    scalars = jnp.stack([part, even]).astype(jnp.int32)
    swap = [(i, i ^ 1) for i in range(number)]
    behind = [(i, (i + CYCLE) % number) for i in range(number)]
    ahead = [(i, (i - CYCLE) % number) for i in range(number)]
    tz = jnp.asarray(plan.table_z())
    ty_forward, ty_backward = (jnp.asarray(t) for t in plan.table_y())
    tx_forward, tx_backward = (jnp.asarray(t) for t in plan.table_x())
    across, within = (jnp.asarray(t) for t in plan.waves())
    chunks = plan.planes // CHUNK
    whole = own.shape
    packed = (CHUNK * plan.packed, LANES)
    pieces = pieces_of(plan.planes)

    (first,) = call(functools.partial(pack_kernel, plan), scalars, (own,), [packed], chunk=(own, 0))
    q, r = [], []

    def shift(chunk):
        q.append(lax.ppermute(chunk, "band", swap))
        r.append(lax.ppermute(chunk, "band", behind))

    shift(first)
    out = call(
        functools.partial(forward_own_kernel, plan),
        scalars,
        (own, tz, ty_forward),
        [(plan.block, LANES)] * parts + [packed] * (chunks - 1),
        (ty_forward,),
        after=first,
    )
    blocks, mine = out[:parts], [first, *out[parts:]]
    own_in = exchange(blocks, parts)
    for c in range(1, chunks):
        shift(mine[c])
    after = blocks[0]
    rows = plan.rows * CHUNK
    pair_in = []
    for c in range(chunks):
        last = c == chunks - 1
        out = call(
            functools.partial(forward_pair_kernel, plan),
            scalars,
            (mine[c], q[c], r[c], tz, ty_forward),
            [(rows, LANES)] * (2 * parts) if last else [(2 * rows, LANES)] * parts,
            (ty_forward,),
            after=after,
        )
        after = out[0]
        if last:
            visit_last = exchange(out[:parts], parts)
            mixed_last = exchange(out[parts:], parts)
        else:
            pair_in.append(exchange(out, parts))
    (screen,) = call(
        functools.partial(screen_kernel, plan),
        scalars,
        (across, within),
        [(plan.rows * plan.length, LANES)],
        (within,),
        after=after,
    )

    def middle(ins, places, sizes, outs, after):
        return call(
            functools.partial(middle_kernel, plan, places, sizes),
            scalars,
            (*[block for part in ins for block in part], screen, tx_forward, tx_backward),
            [(plan.block, LANES)] * 2 + outs,
            (tx_forward, tx_backward),
            after=after,
        )

    own_mid = middle(
        [[b] for b in own_in],
        ((plan.planes, 0),),
        (plan.planes,),
        [(plan.block, LANES)] * (parts - 2),
        screen,
    )

    def middle_of(last, half, arrays, after):
        base = plan.rows * CHUNK if half == 0 else 0
        outs = []
        for i in range(parts - 2):
            for c, size in enumerate(pieces):
                n = plan.rows * size
                if c == 0:
                    outs.append((n, LANES))
                else:
                    array = None if arrays is None else arrays[i * len(pieces) + c]
                    outs.append(Block((2 * n, LANES), n, half, array))
        return middle(
            [[*(pair_in[c][k] for c in range(chunks - 1)), last[k]] for k in range(parts)],
            ((CHUNK, base),) * (chunks - 1) + ((CHUNK, 0),),
            pieces,
            outs,
            after,
        )

    mixed_mid = middle_of(mixed_last, 0, None, own_mid[0])
    mixed_far = mixed_mid[2:]
    mixed_first = send_far(mixed_far[:: len(pieces)], parts)
    mixed_near = send(mixed_mid[1], 1, parts)
    visit_mid = middle_of(visit_last, 1, mixed_far, mixed_mid[0])
    visit_far = visit_mid[2:]
    visit_first = send_far(visit_far[:: len(pieces)], parts)
    visit_near = send(visit_mid[1], 1, parts)
    far = [[*mixed_first, *visit_first]]
    for c in range(1, len(pieces)):
        far.append(send_far(visit_far[c :: len(pieces)], parts))
    own_back = exchange(own_mid, parts)
    after = visit_mid[0]
    totals, from_y, from_z = [], [], []
    for c, size in enumerate(pieces):
        piece = (size * plan.packed, LANES)
        total, y, z = call(
            functools.partial(backward_pair_kernel, plan, pieces, c),
            scalars,
            (
                mixed_mid[0],
                mixed_near,
                visit_mid[0],
                visit_near,
                *far[c],
                *mine,
                *q,
                *r,
                tz,
                ty_backward,
            ),
            [piece] * 3,
            (ty_backward,),
            after=after,
        )
        after = total
        totals.append(total)
        from_z.append(lax.ppermute(z, "band", ahead))
        from_y.append(lax.ppermute(y, "band", swap))
    ready = len(pieces) - LATE
    partial, *rest = call(
        functools.partial(backward_own_kernel, plan, pieces),
        scalars,
        (
            *own_back,
            *totals,
            *mine,
            *[part[c] for c in range(ready) for part in (from_y, from_z)],
            tz,
            ty_backward,
        ),
        [whole] + [(size * plan.packed, LANES) for size in pieces[ready:]],
        (ty_backward,),
        after=after,
    )
    late = sum(pieces[ready:])
    (result,) = call(
        functools.partial(final_kernel, plan),
        scalars,
        (*rest, *from_y[ready:], *from_z[ready:]),
        [Block(whole, late, whole[0] // late - 1, partial)],
    )
    return result[None]


def solution(mesh):
    return jax.shard_map(
        exchange_term,
        mesh=mesh,
        in_specs=(P("band", "grid", None, None),),
        out_specs=P("band", "grid", None, None),
        check_vma=False,
    )
```

```python
import functools
from typing import NamedTuple

import jax
import jax.numpy as jnp
import numpy as np
from jax import lax
from jax.experimental import pallas as pl
from jax.experimental.pallas import tpu as pltpu
from jax.sharding import PartitionSpec as P


CYCLE = 2
LANES = 128
F32 = jnp.float32
BF16 = jnp.bfloat16


def cas(rows, columns, length):
    phases = (np.asarray(rows)[:, None] * np.asarray(columns)[None, :]) % length
    angles = 2.0 * np.pi * phases / length
    return np.cos(angles) + np.sin(angles)


def halves(table):
    high = np.asarray(table, np.float32).astype(jnp.bfloat16)
    low = (np.asarray(table, np.float64) - np.asarray(high, np.float64)).astype(np.float32)
    return high, low.astype(jnp.bfloat16)


def doubled(high, low):
    return np.concatenate(
        [np.concatenate([high, high], axis=1), np.concatenate([low, np.zeros_like(low)], axis=1)],
        axis=0,
    )


def wavenumber_sq(indices, length):
    folded = np.minimum(indices, length - indices).astype(np.float32)
    scaled = folded * np.float32(2.0 * np.pi / length)
    return scaled * scaled


class Plan:
    def __init__(self, planes, height, breadth, parts):
        self.planes, self.height, self.breadth, self.parts = planes, height, breadth, parts
        self.length = planes * parts
        self.share = height // parts
        third = breadth // 3
        assert third * 4 == LANES and self.share % 4 == 0 and planes % 8 == 0
        self.third = third
        self.extra = self.share // 4
        self.rows = 3 * self.extra
        assert self.extra <= 8
        self.block = self.rows * planes
        self.packed = 3 * height // 4

    def table_z(self):
        high, low = halves(cas(np.arange(self.breadth), np.arange(self.breadth), self.breadth))
        out = np.zeros((2 * LANES, 2 * LANES), jnp.bfloat16)
        n = self.breadth
        out[:n, :n] = high
        out[:n, LANES : LANES + n] = low
        out[LANES : LANES + n, :n] = high
        return out

    def positions(self, part):
        rows, index = [], []
        for k in range(self.parts):
            base = self.share * (part ^ k)
            for t in range(3):
                for q in range(self.extra):
                    rows.append((k * 3 + t) * 8 + q)
                    index.append(base + t * self.extra + q)
            for q in range(self.extra):
                rows.append((self.parts * 3 + k) * 8 + q)
                index.append(base + 3 * self.extra + q)
        return np.array(rows), np.array(index)

    def table_y(self):
        m = self.parts * 32
        forward, backward = [], []
        for part in range(self.parts):
            rows, index = self.positions(part)
            full = np.zeros((m, self.height))
            full[rows] = cas(index, np.arange(self.height), self.height)
            high, low = halves(full)
            forward.append(doubled(high, low))
            backward.append(doubled(high.T, low.T))
        return np.stack(forward), np.stack(backward)

    def table_x(self):
        forward, backward = [], []
        for part in range(self.parts):
            order = np.concatenate(
                [np.arange(self.planes) + self.planes * (part ^ k) for k in range(self.parts)]
            )
            high, low = halves(cas(np.arange(self.length), order, self.length))
            forward.append(doubled(high, low))
            backward.append(doubled(high.T, low.T))
        return np.stack(forward), np.stack(backward)

    def waves(self):
        across = np.broadcast_to(
            wavenumber_sq(np.arange(self.length), self.length)[:, None], (self.length, LANES)
        )
        row = np.arange(self.rows)[:, None]
        lane = np.arange(LANES)[None, :]
        main = lane < self.breadth
        y = np.where(main, row, 3 * self.extra + row % self.extra)
        z = np.where(main, lane, self.third * (row // self.extra) + lane - self.breadth)
        within = np.zeros((self.parts, -(-self.rows // 8) * 8, LANES), np.float32)
        for part in range(self.parts):
            within[part, : self.rows] = wavenumber_sq(
                part * self.share + y, self.height
            ) + wavenumber_sq(z, self.breadth)
        return np.array(across), within


def split(value):
    high = value.astype(BF16)
    return high, (value - high.astype(F32)).astype(BF16)


def dot(a, b):
    return jnp.dot(a, b, preferred_element_type=F32)


def lanes(shape):
    return lax.broadcasted_iota(jnp.int32, shape, len(shape) - 1)


def along_rows(table, value):
    both = dot(table, jnp.concatenate(split(value), axis=0))
    half = both.shape[0] // 2
    return both[:half] + both[half:]


def along_lanes(value, table):
    both = dot(jnp.concatenate(split(value), axis=1), table)
    return both[:, :LANES] + both[:, LANES:]


def widen(value):
    rows, width = value.shape
    return jnp.concatenate([value, jnp.zeros((rows, LANES - width), value.dtype)], axis=1)


def pack(wide, plan):
    h = plan.height // 4
    tail = wide[3 * h :]
    parts = []
    for t in range(3):
        main = wide[t * h : (t + 1) * h]
        moved = pltpu.roll(tail, plan.breadth - plan.third * t, 1)
        parts.append(jnp.where(lanes(main.shape) < plan.breadth, main, moved))
    return jnp.concatenate(parts, axis=0)


def thirds(parts, plan):
    tail = None
    for t, part in enumerate(parts):
        moved = pltpu.roll(part, (plan.third * (t + 1)) % LANES, 1)
        tail = moved if tail is None else jnp.where(lanes(part.shape) < plan.third * t, tail, moved)
    return tail


def unpack(value, plan):
    h = plan.height // 4
    return jnp.concatenate(
        [value, thirds([value[t * h : (t + 1) * h] for t in range(3)], plan)], axis=0
    )


def store_spectrum(plan, density, tz, ty, outs, base, stride, plane):
    h, e = plan.height, plan.extra
    once = along_lanes(density, tz)
    for pair in range(CHUNK // 2):
        two = jnp.concatenate(
            [once[(2 * pair + i) * h : (2 * pair + i + 1) * h] for i in range(2)], axis=1
        )
        spectrum = along_rows(ty, two)
        for i in range(2):
            s = spectrum[:, i * LANES : (i + 1) * LANES]
            for k in range(plan.parts):
                tail = s[(3 * plan.parts + k) * 8 : (3 * plan.parts + k + 1) * 8]
                for t in range(3):
                    main = s[(k * 3 + t) * 8 : (k * 3 + t + 1) * 8]
                    moved = pltpu.roll(tail, plan.breadth - plan.third * t, 1)
                    packed = jnp.where(lanes(main.shape) < plan.breadth, main, moved)
                    first = base + t * e * stride + plane + 2 * pair + i
                    outs[k][pl.ds(first, e, stride=stride), :] = packed[:e]


def load_potential(plan, place, planes, tz, ty):
    e = plan.extra
    found = []
    for first in range(0, len(planes), 2):
        two = []
        for plane in planes[first : first + 2]:
            rows, tails = [], []
            for ref, stride, offset in place(plane):
                parts = []
                for t in range(3):
                    at = t * e * stride + offset
                    part = ref[pl.ds(at, e, stride=stride), :]
                    parts.append(jnp.concatenate([part, jnp.zeros((8 - e, LANES), F32)], axis=0))
                rows += parts
                tails.append(thirds(parts, plan))
            two.append(jnp.concatenate(rows + tails, axis=0))
        once = along_rows(ty, jnp.concatenate(two, axis=1))
        found += [once[:, :LANES], once[:, LANES:]]
    return along_lanes(jnp.concatenate(found, axis=0), tz)


CHUNK = 8
PIECES = 3
LATE = 1


def pack_kernel(plan, ins, outs):
    for i in range(CHUNK):
        outs[0][i * plan.packed : (i + 1) * plan.packed, :] = pack(widen(ins[0][i]), plan)


def unpack_chunk(value, plan):
    return jnp.concatenate(
        [unpack(value[i * plan.packed : (i + 1) * plan.packed], plan) for i in range(CHUNK)],
        axis=0,
    )


def pack_chunk(wide, plan):
    h = plan.height
    return jnp.concatenate(
        [pack(wide[i * h : (i + 1) * h], plan) for i in range(wide.shape[0] // h)], axis=0
    )


def planes_of(refs, first, size, plan):
    parts = []
    while size:
        c, at = divmod(first, CHUNK)
        count = min(size, CHUNK - at)
        parts.append(refs[c][at * plan.packed : (at + count) * plan.packed, :])
        first, size = first + count, size - count
    return jnp.concatenate(parts, axis=0)


def forward_own_kernel(plan, ins, outs):
    own_ref, tz_ref, ty_ref = ins
    blocks, later = outs[: plan.parts], outs[plan.parts :]
    for c in range(plan.planes // CHUNK):
        here = slice(c * CHUNK, (c + 1) * CHUNK)
        wide = widen(own_ref[here].reshape(CHUNK * plan.height, plan.breadth))
        if c:
            later[c - 1][...] = pack_chunk(wide, plan)
        store_spectrum(
            plan, wide * wide, tz_ref[...], ty_ref[lax.axis_index("grid")], blocks, 0, plan.planes, c * CHUNK
        )


def forward_pair_kernel(plan, ins, outs):
    p_ref, q_ref, r_ref, tz_ref, ty_ref = ins
    even = lax.axis_index("band") % 2 == 1
    p, r = p_ref[...], r_ref[...]
    tz, ty = tz_ref[...], ty_ref[lax.axis_index("grid")]
    apart = len(outs) > plan.parts
    blocks, base = (outs[plan.parts :], 0) if apart else (outs, plan.rows * CHUNK)
    mixed = q_ref[...] * jnp.where(even, r, p)
    store_spectrum(plan, unpack_chunk(mixed, plan), tz, ty, blocks, base, CHUNK, 0)
    store_spectrum(plan, unpack_chunk(p * r, plan), tz, ty, outs[: plan.parts], 0, CHUNK, 0)


def screen_kernel(plan, ins, outs):
    across_ref, within_ref = ins
    part = lax.axis_index("grid")
    cells = plan.length * plan.height * plan.breadth
    limit = 4.0 * np.pi / plan.length
    rate = 1.0 / (4.0 * limit * limit)
    for row in range(plan.rows):
        wave_sq = across_ref[...] + within_ref[part, row : row + 1, :]
        guarded = jnp.where(wave_sq > 0, wave_sq, 1.0)
        screened = (-0.2 * 4.0 * np.pi / cells) / guarded * (1.0 - jnp.exp(guarded * -rate))
        outs[0][row * plan.length : (row + 1) * plan.length, :] = jnp.where(
            wave_sq > 0, screened, 0.0
        )


def middle_kernel(plan, chunks, sizes, ins, outs):
    n, length = plan.parts, plan.length
    blocks = [ins[k * len(chunks) : (k + 1) * len(chunks)] for k in range(n)]
    screen_ref, tf_ref, tb_ref = ins[n * len(chunks) :]
    part = lax.axis_index("grid")
    tf, tb = tf_ref[part], tb_ref[part]
    cut = [outs[2 + i * len(sizes) : 2 + (i + 1) * len(sizes)] for i in range(n - 2)]
    for pair in range(plan.rows // 2):
        columns = []
        for row in (pair * 2, pair * 2 + 1):
            parts = []
            for block in blocks:
                for ref, (size, base) in zip(block, chunks):
                    parts.append(ref[base + row * size : base + (row + 1) * size, :])
            columns.append(jnp.concatenate(parts, axis=0))
        spectrum = along_rows(tf, jnp.concatenate(columns, axis=1))
        screen = jnp.concatenate(
            [
                screen_ref[row * length : (row + 1) * length, :]
                for row in (pair * 2, pair * 2 + 1)
            ],
            axis=1,
        )
        back = along_rows(tb, spectrum * screen)
        for i in range(2):
            row, lane = pair * 2 + i, slice(i * LANES, (i + 1) * LANES)
            for k in range(n):
                at = k * plan.planes
                refs = cut[k - 2] if k >= 2 else outs[k : k + 1]
                for ref, size in zip(refs, sizes if k >= 2 else (plan.planes,)):
                    ref[row * size : (row + 1) * size, :] = back[at : at + size, lane]
                    at += size


def backward_pair_kernel(plan, pieces, piece, ins, outs):
    far = plan.parts - 2
    whole, ins = ins[:4], ins[4:]
    apart = piece == 0
    blocks, ins = ins[: far * (1 + apart)], ins[far * (1 + apart) :]
    chunks = plan.planes // CHUNK
    first, size = sum(pieces[:piece]), pieces[piece]
    p, q, r = (
        planes_of(ins[i * chunks : (i + 1) * chunks], first, size, plan) for i in range(3)
    )
    tz, ty = ins[3 * chunks][...], ins[3 * chunks + 1][lax.axis_index("grid")]
    even = lax.axis_index("band") % 2 == 1

    def solved(which):
        base = 0 if apart else which * plan.rows * size
        refs = blocks[which * far : (which + 1) * far] if apart else blocks

        def place(i):
            near = [(ref, plan.planes, first + i) for ref in whole[2 * which : 2 * which + 2]]
            return near + [(ref, size, base + i) for ref in refs]

        return pack_chunk(load_potential(plan, place, range(size), tz, ty), plan)

    mixed, visit = solved(0), solved(1)
    total_ref, y_ref, z_ref = outs
    other = mixed * q
    zero = jnp.zeros_like(other)
    y_ref[...] = mixed * jnp.where(even, r, p)
    z_ref[...] = visit * p + jnp.where(even, other, zero)
    total_ref[...] = visit * r + jnp.where(even, zero, other)


def store_result(out_ref, first, value, plan):
    for i in range(value.shape[0] // plan.packed):
        wide = unpack(value[i * plan.packed : (i + 1) * plan.packed], plan)
        out_ref[first + i] = wide[:, : plan.breadth]


def backward_own_kernel(plan, pieces, ins, outs):
    n, count, chunks = plan.parts, len(pieces), plan.planes // CHUNK
    ready = count - LATE
    blocks, ins = ins[:n], ins[n:]
    totals, ins = ins[:count], ins[count:]
    owns, ins = ins[:chunks], ins[chunks:]
    returned, (tz_ref, ty_ref) = ins[: 2 * ready], ins[2 * ready :]
    out_ref, *rest = outs

    def place(plane):
        return [(ref, plan.planes, plane) for ref in blocks]

    first = 0
    for c, size in enumerate(pieces):
        value = load_potential(plan, place, range(first, first + size), tz_ref[...], ty_ref[lax.axis_index("grid")])
        value = pack_chunk(value, plan) * planes_of(owns, first, size, plan) + totals[c][...]
        if c < ready:
            value = value + returned[2 * c][...] + returned[2 * c + 1][...]
            store_result(out_ref, first, value, plan)
        else:
            rest[c - ready][...] = value
        first += size


def final_kernel(plan, ins, outs):
    rest, ys, zs = ins[:LATE], ins[LATE : 2 * LATE], ins[2 * LATE :]
    first = 0
    for part, y, z in zip(rest, ys, zs):
        store_result(outs[0], first, part[...] + y[...] + z[...], plan)
        first += part.shape[0] // plan.packed


class Block(NamedTuple):
    shape: tuple
    rows: int
    index: int
    array: jax.Array | None = None


def call(kernel, operands, outs, chunk=None, after=None):
    specs = []
    for operand in operands:
        shape, first = operand.shape, 0
        if chunk is not None and operand is chunk[0]:
            shape, first = (CHUNK,) + shape[1:], chunk[1]
        at = (first,) + (0,) * (operand.ndim - 1)
        specs.append(pl.BlockSpec(shape, lambda i, at=at: at))
    count = len(operands)
    extras = [] if after is None else [after]
    out_specs, shapes, aliases = [], [], {}
    for i, out in enumerate(outs):
        if not isinstance(out, Block):
            out = Block(out, out[0], 0)
        if out.array is not None:
            aliases[count + len(extras)] = i
            extras.append(out.array)
        shapes.append(jax.ShapeDtypeStruct(out.shape, F32))
        at = (out.index,) + (0,) * (len(out.shape) - 1)
        out_specs.append(pl.BlockSpec((out.rows,) + out.shape[1:], lambda i, at=at: at))
    seen = count + len(extras)

    def body(*refs):
        kernel(refs[:count], refs[seen:])

    return pl.pallas_call(
        body,
        grid=(1,),
        in_specs=specs + [pl.BlockSpec(memory_space=pl.ANY)] * len(extras),
        out_specs=out_specs,
        input_output_aliases=aliases,
        out_shape=shapes,
        compiler_params=pltpu.CompilerParams(vmem_limit_bytes=48 * 1024 * 1024),
    )(*operands, *extras)


def send(block, k, parts):
    return lax.ppermute(block, "grid", [(i, i ^ k) for i in range(parts)])


def send_far(blocks, parts):
    return [send(block, k, parts) for k, block in zip(range(2, parts), blocks)]


def exchange(blocks, parts):
    far = send_far(blocks[2:], parts)
    return [blocks[0], send(blocks[1], 1, parts), *far]


def pieces_of(planes):
    return (planes // PIECES,) * PIECES


def exchange_term(bands):
    parts = lax.axis_size("grid")
    number = lax.axis_size("band")
    own = bands[0]
    plan = Plan(*own.shape, parts)
    swap = [(i, i ^ 1) for i in range(number)]
    behind = [(i, (i + CYCLE) % number) for i in range(number)]
    ahead = [(i, (i - CYCLE) % number) for i in range(number)]
    tz = jnp.asarray(plan.table_z())
    ty_forward, ty_backward = (jnp.asarray(t) for t in plan.table_y())
    tx_forward, tx_backward = (jnp.asarray(t) for t in plan.table_x())
    across, within = (jnp.asarray(t) for t in plan.waves())
    chunks = plan.planes // CHUNK
    whole = own.shape
    packed = (CHUNK * plan.packed, LANES)
    pieces = pieces_of(plan.planes)

    (first,) = call(functools.partial(pack_kernel, plan), (own,), [packed], chunk=(own, 0))
    q, r = [], []

    def shift(chunk):
        q.append(lax.ppermute(chunk, "band", swap))
        r.append(lax.ppermute(chunk, "band", behind))

    shift(first)
    out = call(
        functools.partial(forward_own_kernel, plan),
        (own, tz, ty_forward),
        [(plan.block, LANES)] * parts + [packed] * (chunks - 1),
        after=first,
    )
    blocks, mine = out[:parts], [first, *out[parts:]]
    own_in = exchange(blocks, parts)
    for c in range(1, chunks):
        shift(mine[c])
    after = blocks[0]
    rows = plan.rows * CHUNK
    pair_in = []
    for c in range(chunks):
        last = c == chunks - 1
        out = call(
            functools.partial(forward_pair_kernel, plan),
                (mine[c], q[c], r[c], tz, ty_forward),
            [(rows, LANES)] * (2 * parts) if last else [(2 * rows, LANES)] * parts,
            after=after,
        )
        after = out[0]
        if last:
            visit_last = exchange(out[:parts], parts)
            mixed_last = exchange(out[parts:], parts)
        else:
            pair_in.append(exchange(out, parts))
    (screen,) = call(
        functools.partial(screen_kernel, plan),
        (across, within),
        [(plan.rows * plan.length, LANES)],
        after=after,
    )

    def middle(ins, places, sizes, outs, after):
        return call(
            functools.partial(middle_kernel, plan, places, sizes),
                (*[block for part in ins for block in part], screen, tx_forward, tx_backward),
            [(plan.block, LANES)] * 2 + outs,
            after=after,
        )

    own_mid = middle(
        [[b] for b in own_in],
        ((plan.planes, 0),),
        (plan.planes,),
        [(plan.block, LANES)] * (parts - 2),
        screen,
    )

    def middle_of(last, half, arrays, after):
        base = plan.rows * CHUNK if half == 0 else 0
        outs = []
        for i in range(parts - 2):
            for c, size in enumerate(pieces):
                n = plan.rows * size
                if c == 0:
                    outs.append((n, LANES))
                else:
                    array = None if arrays is None else arrays[i * len(pieces) + c]
                    outs.append(Block((2 * n, LANES), n, half, array))
        return middle(
            [[*(pair_in[c][k] for c in range(chunks - 1)), last[k]] for k in range(parts)],
            ((CHUNK, base),) * (chunks - 1) + ((CHUNK, 0),),
            pieces,
            outs,
            after,
        )

    mixed_mid = middle_of(mixed_last, 0, None, own_mid[0])
    mixed_far = mixed_mid[2:]
    mixed_first = send_far(mixed_far[:: len(pieces)], parts)
    mixed_near = send(mixed_mid[1], 1, parts)
    visit_mid = middle_of(visit_last, 1, mixed_far, mixed_mid[0])
    visit_far = visit_mid[2:]
    visit_first = send_far(visit_far[:: len(pieces)], parts)
    visit_near = send(visit_mid[1], 1, parts)
    far = [[*mixed_first, *visit_first]]
    for c in range(1, len(pieces)):
        far.append(send_far(visit_far[c :: len(pieces)], parts))
    own_back = exchange(own_mid, parts)
    after = visit_mid[0]
    totals, from_y, from_z = [], [], []
    for c, size in enumerate(pieces):
        piece = (size * plan.packed, LANES)
        total, y, z = call(
            functools.partial(backward_pair_kernel, plan, pieces, c),
                (
                mixed_mid[0],
                mixed_near,
                visit_mid[0],
                visit_near,
                *far[c],
                *mine,
                *q,
                *r,
                tz,
                ty_backward,
            ),
            [piece] * 3,
            after=after,
        )
        after = total
        totals.append(total)
        from_z.append(lax.ppermute(z, "band", ahead))
        from_y.append(lax.ppermute(y, "band", swap))
    ready = len(pieces) - LATE
    partial, *rest = call(
        functools.partial(backward_own_kernel, plan, pieces),
        (
            *own_back,
            *totals,
            *mine,
            *[part[c] for c in range(ready) for part in (from_y, from_z)],
            tz,
            ty_backward,
        ),
        [whole] + [(size * plan.packed, LANES) for size in pieces[ready:]],
        after=after,
    )
    late = sum(pieces[ready:])
    (result,) = call(
        functools.partial(final_kernel, plan),
        (*rest, *from_y[ready:], *from_z[ready:]),
        [Block(whole, late, whole[0] // late - 1, partial)],
    )
    return result[None]


def solution(mesh):
    return jax.shard_map(
        exchange_term,
        mesh=mesh,
        in_specs=(P("band", "grid", None, None),),
        out_specs=P("band", "grid", None, None),
        check_vma=False,
    )
```
